64 devices in a mesh: dp: 4 (over x, y), tp: 16 (over z, core).
Axes of the slice: x: 2, y: 2, z: 8, core: 2. Of those that a mesh axis runs over, the one named last changes fastest.
The devices are a block of a 4x4x8 slice.
Arguments:
- x_in: bfloat16 [16384, 1024], P(('dp', 'tp')), parts along dimension 0
- doc_ids: int32 [16384], P(('dp', 'tp')), parts along dimension 0
- doc_pos: int32 [16384], P(('dp', 'tp')), parts along dimension 0
- gamma1: bfloat16 [1024], replicated
- w_qkv: bfloat16 [1024, 3, 1024], P(None, None, 'tp')
- w_out: bfloat16 [1024, 1024], P('tp')
- gamma2: bfloat16 [1024], replicated
- w_in: bfloat16 [1024, 2, 2624], P(None, None, 'tp')
- w_down: bfloat16 [2624, 1024], P('tp')
- grad_out: bfloat16 [16384, 1024], P(('dp', 'tp')), parts along dimension 0
Outputs:
- output 1: bfloat16 [16384, 1024], P(('dp', 'tp')), parts along dimension 0
- output 2: bfloat16 [16384, 1024], P(('dp', 'tp')), parts along dimension 0
- output 3: float32 [4096], P('dp'), parts along dimension 0
- output 4: float32 [4096, 3, 1024], P('dp', None, 'tp'), parts along dimension 0
- output 5: float32 [4096, 1024], P(('dp', 'tp')), parts along dimension 0
- output 6: float32 [4096], P('dp'), parts along dimension 0
- output 7: float32 [4096, 2, 2624], P('dp', None, 'tp'), parts along dimension 0
- output 8: float32 [10496, 1024], P(('dp', 'tp')), parts along dimension 0
There are 4 independent parts. The reference program is written for one: setup_inputs(seed, part) draws one part's arguments, and reference() takes and returns one part's arrays. A program takes and returns all parts, laid end to end along the dimension named above; an argument that names none is the same for every part.
All inputs are finite; a program needn't handle non-finite values.
Results may differ from the reference program's by a relative error of at most 0.02.
Values are sent between devices in bfloat16 or wider.
A program may use at most 768 MiB of HBM per device.

```python
import jax
import jax.numpy as jnp
from jax import lax

MODEL_DIM = 1024
N_HEADS = 16
FF_DIM = 2624
TOKENS = 4096
HEAD_DIM = 64
MAX_DOC = 512


def draw_docs(doc_key):
    num_docs = TOKENS // 16 + 2
    lengths = jax.random.randint(doc_key, (num_docs,), 16, MAX_DOC + 1, dtype=jnp.int32)
    lengths = lengths.at[1].set(MAX_DOC)
    doc_ends = jnp.cumsum(lengths).astype(jnp.int32)
    tok_index = jnp.arange(TOKENS, dtype=jnp.int32)
    doc_ids = jnp.searchsorted(doc_ends, tok_index, side='right').astype(jnp.int32)
    doc_starts = doc_ends - lengths
    doc_pos = tok_index - doc_starts[doc_ids]
    return doc_ids, doc_pos


def setup_inputs(seed: int = 0, part: int = 0) -> dict:
    part_key = jax.random.fold_in(jax.random.key(seed), part)
    key_x, key_doc, key_grad = jax.random.split(part_key, 3)
    shared = jax.random.split(jax.random.key(seed + 1), 6)
    doc_ids, doc_pos = draw_docs(key_doc)
    x_in = jax.random.normal(key_x, (TOKENS, MODEL_DIM), jnp.float32)
    gamma1 = 1.0 + 0.2 * jax.random.normal(shared[0], (MODEL_DIM,), jnp.float32)
    w_qkv = jax.random.normal(shared[1], (MODEL_DIM, 3, MODEL_DIM), jnp.float32) * MODEL_DIM ** -0.5
    w_out = jax.random.normal(shared[2], (MODEL_DIM, MODEL_DIM), jnp.float32) * MODEL_DIM ** -0.5
    gamma2 = 1.0 + 0.2 * jax.random.normal(shared[3], (MODEL_DIM,), jnp.float32)
    w_in = jax.random.normal(shared[4], (MODEL_DIM, 2, FF_DIM), jnp.float32) * MODEL_DIM ** -0.5
    w_down = jax.random.normal(shared[5], (FF_DIM, MODEL_DIM), jnp.float32) * FF_DIM ** -0.5
    grad_out = jax.random.normal(key_grad, (TOKENS, MODEL_DIM), jnp.float32)
    return {'x_in': x_in.astype(jnp.bfloat16), 'doc_ids': doc_ids, 'doc_pos': doc_pos,
            'gamma1': gamma1.astype(jnp.bfloat16), 'w_qkv': w_qkv.astype(jnp.bfloat16),
            'w_out': w_out.astype(jnp.bfloat16), 'gamma2': gamma2.astype(jnp.bfloat16),
            'w_in': w_in.astype(jnp.bfloat16), 'w_down': w_down.astype(jnp.bfloat16),
            'grad_out': grad_out.astype(jnp.bfloat16)}


def layer_norm(values, gain):
    vals32 = values.astype(jnp.float32)
    mean_val = jnp.mean(vals32, axis=-1, keepdims=True)
    centered = vals32 - mean_val
    var_val = jnp.mean(centered * centered, axis=-1, keepdims=True)
    return (centered * lax.rsqrt(var_val + 1e-5) * gain).astype(jnp.bfloat16)


def rope_tables(doc_pos):
    half_dim = HEAD_DIM // 2
    inv_freq = 160000.0 ** (-jnp.arange(half_dim, dtype=jnp.float32) / half_dim)
    angle = doc_pos.astype(jnp.float32)[:, None] * inv_freq[None, :]
    angle = jnp.concatenate([angle, angle], axis=-1)[:, None, :]
    return jnp.cos(angle), jnp.sin(angle)


def rotate(head_vals, cos_t, sin_t):
    vals32 = head_vals.astype(jnp.float32)
    half_dim = HEAD_DIM // 2
    turned = jnp.concatenate([-vals32[..., half_dim:], vals32[..., :half_dim]], axis=-1)
    return (vals32 * cos_t + turned * sin_t).astype(jnp.bfloat16)


def window_stack(padded, block_len, num_shift, num_blocks):
    pieces = [padded[shift * block_len: shift * block_len + num_blocks * block_len].reshape((num_blocks, block_len) + padded.shape[1:]) for shift in range(num_shift)]
    return jnp.concatenate(pieces, axis=1)


def attention(q_rot, k_rot, v_val, doc_ids):
    num_blocks = TOKENS // MAX_DOC
    pad_rows = ((MAX_DOC, MAX_DOC), (0, 0), (0, 0))
    k_win = window_stack(jnp.pad(k_rot, pad_rows), MAX_DOC, 3, num_blocks)
    v_win = window_stack(jnp.pad(v_val, pad_rows), MAX_DOC, 3, num_blocks)
    seg_win = window_stack(jnp.pad(doc_ids, (MAX_DOC, MAX_DOC), constant_values=-1), MAX_DOC, 3, num_blocks)
    q_blk = q_rot.reshape(num_blocks, MAX_DOC, N_HEADS, HEAD_DIM)
    seg_blk = doc_ids.reshape(num_blocks, MAX_DOC)

    def one_block(block_args):
        q_b, k_b, v_b, seg_q, seg_k = block_args
        score = jnp.einsum('qhe,khe->hqk', q_b.astype(jnp.float32), k_b.astype(jnp.float32)) * 0.125
        same_doc = seg_q[None, :, None] == seg_k[None, None, :]
        score = jnp.where(same_doc, score, -1e30)
        attn_prob = jax.nn.softmax(score, axis=-1).astype(jnp.bfloat16)
        mixed = jnp.einsum('hqk,khe->qhe', attn_prob.astype(jnp.float32), v_b.astype(jnp.float32))
        return mixed.astype(jnp.bfloat16)

    result = lax.map(jax.checkpoint(one_block), (q_blk, k_win, v_win, seg_blk, seg_win))
    return result.reshape(TOKENS, N_HEADS * HEAD_DIM)


def reference(x_in, doc_ids, doc_pos, gamma1, w_qkv, w_out, gamma2, w_in, w_down, grad_out):
    cos_t, sin_t = rope_tables(doc_pos)

    def forward(x_val, gain_one, wqkv_f32, wout_f32, gain_two, win_f32, wdown_f32):
        normed = layer_norm(x_val, gain_one)
        qkv_vals = jnp.einsum('td,dcn->tcn', normed.astype(jnp.float32), wqkv_f32).astype(jnp.bfloat16)
        qkv_vals = qkv_vals.reshape(TOKENS, 3, N_HEADS, HEAD_DIM)
        q_rot = rotate(qkv_vals[:, 0], cos_t, sin_t)
        k_rot = rotate(qkv_vals[:, 1], cos_t, sin_t)
        mixed = attention(q_rot, k_rot, qkv_vals[:, 2], doc_ids)
        att_proj = jnp.dot(mixed.astype(jnp.float32), wout_f32, preferred_element_type=jnp.float32).astype(jnp.bfloat16)
        hidden = (x_val.astype(jnp.float32) + att_proj.astype(jnp.float32)).astype(jnp.bfloat16)
        normed_two = layer_norm(hidden, gain_two)
        gate_pair = jnp.einsum('td,dcf->tcf', normed_two.astype(jnp.float32), win_f32).astype(jnp.bfloat16)
        gated = (jax.nn.gelu(gate_pair[:, 0].astype(jnp.float32), approximate=False) * gate_pair[:, 1].astype(jnp.float32)).astype(jnp.bfloat16)
        mlp_proj = jnp.dot(gated.astype(jnp.float32), wdown_f32, preferred_element_type=jnp.float32).astype(jnp.bfloat16)
        return (hidden.astype(jnp.float32) + mlp_proj.astype(jnp.float32)).astype(jnp.bfloat16)

    layer_out, pullback = jax.vjp(forward, x_in, gamma1.astype(jnp.float32), w_qkv.astype(jnp.float32),
                                  w_out.astype(jnp.float32), gamma2.astype(jnp.float32),
                                  w_in.astype(jnp.float32), w_down.astype(jnp.float32))
    grad_x, grad_gamma1, grad_w_qkv, grad_w_out, grad_gamma2, grad_w_in, grad_w_down = pullback(grad_out)
    return (layer_out, grad_x, grad_gamma1, grad_w_qkv, grad_w_out, grad_gamma2, grad_w_in, grad_w_down)
```

```python
import math
import jax
import jax.numpy as jnp
from jax import lax
from jax.experimental import pallas as pl
from jax.experimental.pallas import tpu as pltpu
from jax.sharding import PartitionSpec as P

MAX_DOC = 512
HEAD_DIM = 64
HALF = HEAD_DIM // 2
FF_ALIGN = 8
MLP_SHARDS = 4
LOG2E = 1.4426950408889634
S_SCALE = 0.125 * LOG2E
NEG = -1e30
SQRT_HALF = 0.7071067811865476
INV_SQRT_2PI = 0.3989422804014327
F32 = jnp.float32
BF16 = jnp.bfloat16


def layer_norm(values, gain):
    vals32 = values.astype(F32)
    mean_val = jnp.mean(vals32, axis=-1, keepdims=True)
    centered = vals32 - mean_val
    var_val = jnp.mean(centered * centered, axis=-1, keepdims=True)
    return (centered * lax.rsqrt(var_val + 1e-5) * gain).astype(BF16)


def dot_nn(a, b):
    return lax.dot_general(a, b, (((1,), (0,)), ((), ())), preferred_element_type=F32)


def dot_nt(a, b):
    return lax.dot_general(a, b, (((1,), (1,)), ((), ())), preferred_element_type=F32)


def dot_tn(a, b):
    return lax.dot_general(a, b, (((0,), (0,)), ((), ())), preferred_element_type=F32)


def flip(vals):
    return vals.astype(F32).T.astype(BF16)


def rope_fwd(vals_t, cos_t, sin_t):
    rows = []
    for head in range(2):
        lo = vals_t[head * HEAD_DIM: head * HEAD_DIM + HALF]
        hi = vals_t[head * HEAD_DIM + HALF: (head + 1) * HEAD_DIM]
        rows += [lo * cos_t - hi * sin_t, hi * cos_t + lo * sin_t]
    return jnp.concatenate(rows, axis=0)


def rope_back(lo, hi, cos_t, sin_t):
    return [lo * cos_t + hi * sin_t, hi * cos_t - lo * sin_t]


def attn_fwd_kernel(halo, tok, x_ref, g1_ref, g2_ref, w_ref, cos_ref, sin_ref, segc_ref, segr_ref,
                    u_ref, qt_ref, kt_ref, vt_ref, ot_ref, lse_ref, hid_ref, n2_ref, bias_ref, att_ref):
    own = pl.ds(halo, tok)
    step = pl.program_id(0)

    @pl.when(step == 0)
    def _():
        u_ref[...] = layer_norm(x_ref[...], g1_ref[...])
        bias_ref[...] = jnp.where(segc_ref[...] == segr_ref[...], 0.0, NEG).astype(F32)
        att_ref[...] = jnp.zeros_like(att_ref)

    wide = w_ref.shape[3]
    w_q, w_k, w_v, w_o = [w_ref[:, part].reshape(2 * HEAD_DIM, wide) for part in range(4)]
    u_win = u_ref[...]
    u_own = u_ref[own, :]
    q_raw = dot_nt(w_q, u_own).astype(BF16).astype(F32)
    k_raw = dot_nt(w_k, u_win).astype(BF16).astype(F32)
    v_t = dot_nt(w_v, u_win).astype(BF16)
    q_t = rope_fwd(q_raw, cos_ref[:, halo:halo + tok], sin_ref[:, halo:halo + tok]).astype(BF16)
    k_t = rope_fwd(k_raw, cos_ref[...], sin_ref[...]).astype(BF16)
    qt_ref[...] = q_t
    kt_ref[...] = k_t
    vt_ref[...] = v_t
    for head in range(2):
        rows = slice(head * HEAD_DIM, (head + 1) * HEAD_DIM)
        score = dot_nn(flip(k_t[rows]), q_t[rows]) * S_SCALE + bias_ref[...]
        top = jnp.max(score, axis=0, keepdims=True)
        expd = jnp.exp2(score - top)
        total = jnp.sum(expd, axis=0, keepdims=True)
        prob = (expd * (1.0 / total)).astype(BF16)
        ot_ref[rows, :] = dot_nn(v_t[rows], prob).astype(BF16)
        lse_ref[0, head:head + 1, :] = top + jnp.log2(total)
    att_ref[...] += dot_nn(flip(ot_ref[...]), w_o)

    @pl.when(step == pl.num_programs(0) - 1)
    def _():
        hidden = (x_ref[own, :].astype(F32) + att_ref[...].astype(BF16).astype(F32)).astype(BF16)
        hid_ref[...] = hidden
        n2_ref[...] = layer_norm(hidden, g2_ref[...])


def mlp_kernel(n2_ref, hid_ref, go_ref, g2_ref, w_ref, g_ref, out_ref, dh_ref, gain_ref, mlp_ref, dn_ref):
    step = pl.program_id(0)

    @pl.when(step == 0)
    def _():
        mlp_ref[...] = jnp.zeros_like(mlp_ref)
        dn_ref[...] = jnp.zeros_like(dn_ref)

    n2 = n2_ref[...]
    g_out = go_ref[...]
    per, _, rows, wide = w_ref.shape
    w_a, w_b, w_d = [w_ref[:, part].reshape(per * rows, wide) for part in range(3)]
    gate = dot_nt(w_a, n2).astype(BF16).astype(F32)
    lin = dot_nt(w_b, n2).astype(BF16).astype(F32)
    cdf = 0.5 * (1.0 + lax.erf(gate * SQRT_HALF))
    act = gate * cdf
    gated = (act * lin).astype(BF16)
    d_gated = dot_nt(w_d, g_out).astype(BF16).astype(F32)
    slope = cdf + gate * (jnp.exp2(gate * gate * (-0.5 * LOG2E)) * INV_SQRT_2PI)
    d_gate = (d_gated * lin * slope).astype(BF16)
    d_lin = (d_gated * act).astype(BF16)
    mlp_ref[...] += dot_nn(flip(gated), w_d)
    dn_ref[...] += dot_nn(flip(d_gate), w_a) + dot_nn(flip(d_lin), w_b)
    g_ref[:, 0] = dot_nn(d_gate, n2).astype(BF16).reshape(per, rows, wide)
    g_ref[:, 1] = dot_nn(d_lin, n2).astype(BF16).reshape(per, rows, wide)
    g_ref[:, 2] = dot_nn(gated, g_out).astype(BF16).reshape(per, rows, wide)

    @pl.when(step == pl.num_programs(0) - 1)
    def _():
        hidden = hid_ref[...].astype(F32)
        out_ref[...] = (hidden + mlp_ref[...].astype(BF16).astype(F32)).astype(BF16)
        d_n2 = dn_ref[...].astype(BF16).astype(F32)
        centered = hidden - jnp.mean(hidden, axis=-1, keepdims=True)
        rstd = lax.rsqrt(jnp.mean(centered * centered, axis=-1, keepdims=True) + 1e-5)
        unit = centered * rstd
        gain_ref[...] = jnp.sum(d_n2 * unit, axis=0, keepdims=True)
        d_unit = d_n2 * g2_ref[...]
        d_hid = rstd * (d_unit - jnp.mean(d_unit, axis=-1, keepdims=True)
                        - unit * jnp.mean(d_unit * unit, axis=-1, keepdims=True))
        dh_ref[...] = (g_out.astype(F32) + d_hid.astype(BF16).astype(F32)).astype(BF16)


def attn_bwd_kernel(halo, tok, u_ref, dh_ref, w_ref, cos_ref, sin_ref, segc_ref, segr_ref,
                    qt_ref, kt_ref, vt_ref, ot_ref, lse_ref, g_ref, du_ref, bias_ref, acc_ref):
    own = pl.ds(halo, tok)
    step = pl.program_id(0)

    @pl.when(step == 0)
    def _():
        bias_ref[...] = jnp.where(segc_ref[...] == segr_ref[...], 0.0, NEG).astype(F32)

    wide = w_ref.shape[3]
    d_hid = dh_ref[...]
    do_t = dot_nt(w_ref[:, 3].reshape(2 * HEAD_DIM, wide), d_hid).astype(BF16)
    o_t = ot_ref[...]
    g_ref[:, 3] = dot_nn(o_t, d_hid).astype(BF16).reshape(2, HEAD_DIM, wide)
    cos_w, sin_w = cos_ref[...], sin_ref[...]
    cos_o, sin_o = cos_ref[:, halo:halo + tok], sin_ref[:, halo:halo + tok]
    dq_rows, dk_rows, dv_rows = [], [], []
    for head in range(2):
        rows = slice(head * HEAD_DIM, (head + 1) * HEAD_DIM)
        q_t, k_t, v_t, d_o = qt_ref[rows, :], kt_ref[rows, :], vt_ref[rows, :], do_t[rows]
        score = dot_nn(flip(k_t), q_t) * S_SCALE + bias_ref[...]
        prob = jnp.exp2(score - lse_ref[0, head:head + 1, :])
        delta = jnp.sum(d_o.astype(F32) * o_t[rows].astype(F32), axis=0, keepdims=True)
        d_prob = dot_nn(flip(v_t), d_o).astype(BF16).astype(F32)
        d_score = (prob * (d_prob - delta)).astype(BF16)
        dv_rows.append(dot_nt(d_o, prob.astype(BF16)).astype(BF16))
        d_q = (dot_nn(k_t, d_score) * 0.125).astype(BF16).astype(F32)
        d_k = (dot_nt(q_t, d_score) * 0.125).astype(BF16).astype(F32)
        dq_rows += rope_back(d_q[:HALF], d_q[HALF:], cos_o, sin_o)
        dk_rows += rope_back(d_k[:HALF], d_k[HALF:], cos_w, sin_w)
    dq_t = jnp.concatenate(dq_rows, axis=0).astype(BF16)
    dk_t = jnp.concatenate(dk_rows, axis=0).astype(BF16)
    dv_t = jnp.concatenate(dv_rows, axis=0)
    u_win = u_ref[...]
    g_ref[:, 0] = dot_nn(dq_t, u_ref[own, :]).astype(BF16).reshape(2, HEAD_DIM, wide)
    g_ref[:, 1] = dot_nn(dk_t, u_win).astype(BF16).reshape(2, HEAD_DIM, wide)
    g_ref[:, 2] = dot_nn(dv_t, u_win).astype(BF16).reshape(2, HEAD_DIM, wide)
    w_q = w_ref[:, 0].reshape(2 * HEAD_DIM, wide)
    w_kv = jnp.concatenate([w_ref[:, 1].reshape(2 * HEAD_DIM, wide), w_ref[:, 2].reshape(2 * HEAD_DIM, wide)], axis=0)
    d_kv = jnp.concatenate([flip(dk_t), flip(dv_t)], axis=1)
    term = dot_nn(d_kv, w_kv)

    @pl.when(step == 0)
    def _():
        acc_ref[...] = term

    @pl.when(step > 0)
    def _():
        acc_ref[...] += term

    acc_ref[own, :] += dot_nn(flip(dq_t), w_q)

    @pl.when(step == pl.num_programs(0) - 1)
    def _():
        du_ref[...] = acc_ref[...].astype(BF16)


def whole(shape):
    return pl.BlockSpec(shape, lambda i: (0,) * len(shape))


def attn_forward(x_win, gain1, gain2, w_att, cos_t, sin_t, seg_col, seg_row, tok):
    win, dim = x_win.shape
    heads = w_att.shape[0]
    pairs = heads // 2
    halo = (win - tok) // 2
    feat = 2 * HEAD_DIM
    return pl.pallas_call(
        lambda *refs: attn_fwd_kernel(halo, tok, *refs),
        grid=(pairs,),
        in_specs=[whole((win, dim)), whole((1, dim)), whole((1, dim)),
                  pl.BlockSpec((2, 4, HEAD_DIM, dim), lambda i: (i, 0, 0, 0)),
                  whole((HALF, win)), whole((HALF, win)), whole((win, 1)), whole((1, tok))],
        out_specs=[whole((win, dim)),
                   pl.BlockSpec((feat, tok), lambda i: (i, 0)),
                   pl.BlockSpec((feat, win), lambda i: (i, 0)),
                   pl.BlockSpec((feat, win), lambda i: (i, 0)),
                   pl.BlockSpec((feat, tok), lambda i: (i, 0)),
                   pl.BlockSpec((1, 2, tok), lambda i: (i, 0, 0)),
                   whole((tok, dim)), whole((tok, dim))],
        out_shape=[jax.ShapeDtypeStruct((win, dim), BF16),
                   jax.ShapeDtypeStruct((heads * HEAD_DIM, tok), BF16),
                   jax.ShapeDtypeStruct((heads * HEAD_DIM, win), BF16),
                   jax.ShapeDtypeStruct((heads * HEAD_DIM, win), BF16),
                   jax.ShapeDtypeStruct((heads * HEAD_DIM, tok), BF16),
                   jax.ShapeDtypeStruct((pairs, 2, tok), F32),
                   jax.ShapeDtypeStruct((tok, dim), BF16),
                   jax.ShapeDtypeStruct((tok, dim), BF16)],
        scratch_shapes=[pltpu.VMEM((win, tok), F32), pltpu.VMEM((tok, dim), F32)],
        compiler_params=pltpu.CompilerParams(dimension_semantics=("arbitrary",), vmem_limit_bytes=40 * 1024 * 1024),
        cost_estimate=pl.CostEstimate(flops=20_000_000_000, bytes_accessed=20_000_000, transcendentals=5_000_000),
        name="attn_fwd",
    )(x_win, gain1, gain2, w_att, cos_t, sin_t, seg_col, seg_row)


def mlp(normed2, hidden, grad_out, gain2, w_mlp):
    tok, dim = normed2.shape
    shards, parts, rows, _ = w_mlp.shape
    per = math.gcd(shards, MLP_SHARDS)
    block = pl.BlockSpec((per, parts, rows, dim), lambda i: (i, 0, 0, 0))
    return pl.pallas_call(
        mlp_kernel,
        grid=(shards // per,),
        in_specs=[whole((tok, dim)), whole((tok, dim)), whole((tok, dim)), whole((1, dim)), block],
        out_specs=[block, whole((tok, dim)), whole((tok, dim)), whole((1, dim))],
        out_shape=[jax.ShapeDtypeStruct(w_mlp.shape, BF16),
                   jax.ShapeDtypeStruct((tok, dim), BF16),
                   jax.ShapeDtypeStruct((tok, dim), BF16),
                   jax.ShapeDtypeStruct((1, dim), F32)],
        scratch_shapes=[pltpu.VMEM((tok, dim), F32), pltpu.VMEM((tok, dim), F32)],
        compiler_params=pltpu.CompilerParams(dimension_semantics=("arbitrary",), vmem_limit_bytes=40 * 1024 * 1024),
        cost_estimate=pl.CostEstimate(flops=20_000_000_000, bytes_accessed=35_000_000, transcendentals=1_500_000),
        name="mlp",
    )(normed2, hidden, grad_out, gain2, w_mlp)


def attn_backward(u_win, d_hid, w_att, cos_t, sin_t, seg_col, seg_row, q_t, k_t, v_t, o_t, lse):
    win, dim = u_win.shape
    tok = d_hid.shape[0]
    heads = w_att.shape[0]
    pairs = heads // 2
    halo = (win - tok) // 2
    feat = 2 * HEAD_DIM
    return pl.pallas_call(
        lambda *refs: attn_bwd_kernel(halo, tok, *refs),
        grid=(pairs,),
        in_specs=[whole((win, dim)), whole((tok, dim)),
                  pl.BlockSpec((2, 4, HEAD_DIM, dim), lambda i: (i, 0, 0, 0)),
                  whole((HALF, win)), whole((HALF, win)), whole((win, 1)), whole((1, tok)),
                  pl.BlockSpec((feat, tok), lambda i: (i, 0)),
                  pl.BlockSpec((feat, win), lambda i: (i, 0)),
                  pl.BlockSpec((feat, win), lambda i: (i, 0)),
                  pl.BlockSpec((feat, tok), lambda i: (i, 0)),
                  pl.BlockSpec((1, 2, tok), lambda i: (i, 0, 0))],
        out_specs=[pl.BlockSpec((2, 4, HEAD_DIM, dim), lambda i: (i, 0, 0, 0)), whole((win, dim))],
        out_shape=[jax.ShapeDtypeStruct((heads, 4, HEAD_DIM, dim), BF16),
                   jax.ShapeDtypeStruct((win, dim), BF16)],
        scratch_shapes=[pltpu.VMEM((win, tok), F32), pltpu.VMEM((win, dim), F32)],
        compiler_params=pltpu.CompilerParams(dimension_semantics=("arbitrary",), vmem_limit_bytes=48 * 1024 * 1024),
        cost_estimate=pl.CostEstimate(flops=40_000_000_000, bytes_accessed=30_000_000, transcendentals=5_000_000),
        name="attn_bwd",
    )(u_win, d_hid, w_att, cos_t, sin_t, seg_col, seg_row, q_t, k_t, v_t, o_t, lse)


def solution(mesh):
    tok_spec = P(('dp', 'tp'), None)
    seq_spec = P(('dp', 'tp'))
    in_specs = (tok_spec, seq_spec, seq_spec, P(None), P(None, None, 'tp'), P('tp', None),
                P(None), P(None, None, 'tp'), P('tp', None), tok_spec)
    out_specs = (tok_spec, tok_spec, P('dp'), P('dp', None, 'tp'), P(('dp', 'tp'), None),
                 P('dp'), P('dp', None, 'tp'), P(('dp', 'tp'), None))
    group = mesh.shape['tp']

    def gather_rows(shard_rows):
        return lax.all_gather(shard_rows, 'tp', axis=0, tiled=True)

    def scatter_rows(part_sum):
        return lax.psum_scatter(part_sum, 'tp', scatter_dimension=0, tiled=True)

    def shift(vals, by):
        return lax.ppermute(vals, 'tp', [(d, d + by) for d in range(group) if 0 <= d + by < group])

    def group_sum(vals):
        span = 1
        while span < group:
            vals = vals + lax.ppermute(vals, 'tp', [(d, d ^ span) for d in range(group)])
            span *= 2
        return vals

    def device_step(x_in, doc_ids, doc_pos, gamma1, w_qkv, w_out, gamma2, w_in, w_down, grad_out):
        tok, dim = x_in.shape
        heads_loc = w_qkv.shape[2] // HEAD_DIM
        ff_loc = w_in.shape[2]
        ff_pad = -(-ff_loc // FF_ALIGN) * FF_ALIGN
        reach = -(-MAX_DOC // tok)
        shifts = [by for by in range(reach, -reach - 1, -1)]

        def window(vals, axis):
            return jnp.concatenate([vals if by == 0 else shift(vals, by) for by in shifts], axis=axis)

        x_win = window(x_in, 0)
        marks = window(jnp.stack([doc_ids + 1, doc_pos]), 1)
        seg_row = doc_ids[None, :] + 1
        seg_col = marks[0][:, None]
        inv_freq = 160000.0 ** (-jnp.arange(HALF, dtype=F32) / HALF)
        angle = marks[1].astype(F32)[None, :] * inv_freq[:, None]
        cos_t, sin_t = jnp.cos(angle), jnp.sin(angle)

        qkv_rows = jnp.transpose(w_qkv.reshape(dim, 3, heads_loc, HEAD_DIM), (2, 1, 3, 0))
        out_rows = w_out.reshape(heads_loc, 1, HEAD_DIM, dim)
        att_rows = jnp.concatenate([qkv_rows, out_rows], axis=1)
        w_att = gather_rows(att_rows.reshape(-1, dim)).reshape(group * heads_loc, 4, HEAD_DIM, dim)
        mlp_rows = jnp.concatenate([jnp.transpose(w_in, (1, 2, 0)), w_down[None]], axis=0)
        mlp_rows = jnp.pad(mlp_rows, ((0, 0), (0, ff_pad - ff_loc), (0, 0)))
        w_mlp = gather_rows(mlp_rows.reshape(3 * ff_pad, dim)).reshape(group, 3, ff_pad, dim)

        gain1 = gamma1.astype(F32)[None, :]
        gain2 = gamma2.astype(F32)[None, :]
        u_win, q_t, k_t, v_t, o_t, lse, hidden, normed2 = attn_forward(
            x_win, gain1, gain2, w_att, cos_t, sin_t, seg_col, seg_row, tok)
        g_mlp, layer_out, d_hidden, g_gain2 = mlp(normed2, hidden, grad_out, gain2, w_mlp)
        g_mlp = scatter_rows(g_mlp.reshape(group * 3 * ff_pad, dim))
        g_att, du_win = attn_backward(u_win, d_hidden, w_att, cos_t, sin_t, seg_col, seg_row,
                                      q_t, k_t, v_t, o_t, lse)
        g_mlp, g_att = lax.optimization_barrier((g_mlp, g_att))
        g_att = scatter_rows(g_att.reshape(group * heads_loc * 4 * HEAD_DIM, dim))
        total = None
        for slot, by in enumerate(shifts):
            piece = du_win[slot * tok:(slot + 1) * tok]
            piece = (piece if by == 0 else shift(piece, -by)).astype(F32)
            total = piece if total is None else total + piece
        _, ln1_back = jax.vjp(layer_norm, x_in, gamma1.astype(F32))
        d_x_ln, g_gain1 = ln1_back(total.astype(BF16))
        grad_x = (d_hidden.astype(F32) + d_x_ln.astype(F32)).astype(BF16)
        gains = group_sum(jnp.stack([g_gain1, g_gain2[0]]))

        g_att = g_att.reshape(heads_loc, 4, HEAD_DIM, dim).astype(F32)
        g_qkv = jnp.transpose(g_att[:, :3], (3, 1, 0, 2)).reshape(dim, 3, heads_loc * HEAD_DIM)
        g_out = g_att[:, 3].reshape(heads_loc * HEAD_DIM, dim)
        g_mlp = g_mlp.reshape(3, ff_pad, dim)[:, :ff_loc].astype(F32)
        g_in = jnp.transpose(g_mlp[:2], (2, 0, 1))
        return (layer_out, grad_x, gains[0], g_qkv, g_out, gains[1], g_in, g_mlp[2])

    return jax.shard_map(device_step, mesh=mesh, in_specs=in_specs, out_specs=out_specs, check_vma=False)
```

```python
import math
import jax
import jax.numpy as jnp
from jax import lax
from jax.experimental import pallas as pl
from jax.experimental.pallas import tpu as pltpu
from jax.sharding import PartitionSpec as P

MAX_DOC = 512
HEAD_DIM = 64
HALF = HEAD_DIM // 2
FF_ALIGN = 8
MLP_SHARDS = 4
HEADS_STEP = 4
EXTRA = 256
STREAMS = 2
LOG2E = 1.4426950408889634
S_SCALE = 0.125 * LOG2E
NEG = -1e30
SQRT_HALF = 0.7071067811865476
INV_SQRT_2PI = 0.3989422804014327
F32 = jnp.float32
BF16 = jnp.bfloat16


def layer_norm(values, gain):
    vals32 = values.astype(F32)
    mean_val = jnp.mean(vals32, axis=-1, keepdims=True)
    centered = vals32 - mean_val
    var_val = jnp.mean(centered * centered, axis=-1, keepdims=True)
    return (centered * lax.rsqrt(var_val + 1e-5) * gain).astype(BF16)


def dot_nn(a, b):
    return lax.dot_general(a, b, (((1,), (0,)), ((), ())), preferred_element_type=F32)


def dot_nt(a, b):
    return lax.dot_general(a, b, (((1,), (1,)), ((), ())), preferred_element_type=F32)


def dot_tn(a, b):
    return lax.dot_general(a, b, (((0,), (0,)), ((), ())), preferred_element_type=F32)


def flip(vals):
    return vals.astype(F32).T.astype(BF16)


def rope_fwd(vals_t, cos_t, sin_t):
    rows = []
    for head in range(vals_t.shape[0] // HEAD_DIM):
        lo = vals_t[head * HEAD_DIM: head * HEAD_DIM + HALF]
        hi = vals_t[head * HEAD_DIM + HALF: (head + 1) * HEAD_DIM]
        rows += [lo * cos_t - hi * sin_t, hi * cos_t + lo * sin_t]
    return jnp.concatenate(rows, axis=0)


def rope_back(lo, hi, cos_t, sin_t):
    return [lo * cos_t + hi * sin_t, hi * cos_t - lo * sin_t]


def attn_fwd_kernel(halo, tok, x_ref, g1_ref, g2_ref, w_ref, cos_ref, sin_ref, segc_ref, segr_ref,
                    u_ref, qt_ref, kt_ref, vt_ref, ot_ref, lse_ref, hid_ref, n2_ref, bias_ref, att_ref):
    own = pl.ds(halo, tok)
    step = pl.program_id(0)

    @pl.when(step == 0)
    def _():
        u_ref[...] = layer_norm(x_ref[...], g1_ref[...])
        bias_ref[...] = jnp.where(segc_ref[...] == segr_ref[...], 0.0, NEG).astype(F32)
        att_ref[...] = jnp.zeros_like(att_ref)

    heads, wide = w_ref.shape[0], w_ref.shape[3]
    w_q, w_k, w_v, w_o = [w_ref[:, part].reshape(heads * HEAD_DIM, wide) for part in range(4)]
    u_win = u_ref[...]
    u_own = u_ref[own, :]
    q_raw = dot_nt(w_q, u_own).astype(BF16).astype(F32)
    k_raw = dot_nt(w_k, u_win).astype(BF16).astype(F32)
    v_t = dot_nt(w_v, u_win).astype(BF16)
    q_t = rope_fwd(q_raw, cos_ref[:, halo:halo + tok], sin_ref[:, halo:halo + tok]).astype(BF16)
    k_t = rope_fwd(k_raw, cos_ref[...], sin_ref[...]).astype(BF16)
    qt_ref[...] = q_t
    kt_ref[...] = k_t
    vt_ref[...] = v_t
    for head in range(heads):
        rows = slice(head * HEAD_DIM, (head + 1) * HEAD_DIM)
        score = dot_nn(flip(k_t[rows]), q_t[rows]) * S_SCALE + bias_ref[...]
        top = jnp.max(score, axis=0, keepdims=True)
        expd = jnp.exp2(score - top)
        total = jnp.sum(expd, axis=0, keepdims=True)
        prob = (expd * (1.0 / total)).astype(BF16)
        ot_ref[rows, :] = dot_nn(v_t[rows], prob).astype(BF16)
        lse_ref[0, head:head + 1, :] = top + jnp.log2(total)
    att_ref[...] += dot_nn(flip(ot_ref[...]), w_o)

    @pl.when(step == pl.num_programs(0) - 1)
    def _():
        hidden = (x_ref[own, :].astype(F32) + att_ref[...].astype(BF16).astype(F32)).astype(BF16)
        hid_ref[...] = hidden
        n2_ref[...] = layer_norm(hidden, g2_ref[...])


def mlp_kernel(n2_ref, hid_ref, go_ref, g2_ref, we_ref, wr_ref, g_ref, out_ref, dh_ref, gain_ref, mlp_ref, dn_ref):
    step = pl.program_id(0)

    @pl.when(step == 0)
    def _():
        mlp_ref[...] = jnp.zeros_like(mlp_ref)
        dn_ref[...] = jnp.zeros_like(dn_ref)

    n2 = n2_ref[...]
    g_out = go_ref[...]
    per, _, rows, wide = g_ref.shape
    lead = we_ref.shape[1] * we_ref.shape[2]
    first, rest = we_ref[...].reshape(per, lead, wide), wr_ref[...]
    w_a = first[:, :rows].reshape(per * rows, wide)
    w_b = jnp.concatenate([first[:, rows:], rest[:, :2 * rows - lead]], axis=1).reshape(per * rows, wide)
    w_d = rest[:, 2 * rows - lead:].reshape(per * rows, wide)
    gate = dot_nt(w_a, n2).astype(BF16).astype(F32)
    lin = dot_nt(w_b, n2).astype(BF16).astype(F32)
    cdf = 0.5 * (1.0 + lax.erf(gate * SQRT_HALF))
    act = gate * cdf
    gated = (act * lin).astype(BF16)
    d_gated = dot_nt(w_d, g_out).astype(BF16).astype(F32)
    slope = cdf + gate * (jnp.exp2(gate * gate * (-0.5 * LOG2E)) * INV_SQRT_2PI)
    d_gate = (d_gated * lin * slope).astype(BF16)
    d_lin = (d_gated * act).astype(BF16)
    mlp_ref[...] += dot_nn(flip(gated), w_d)
    dn_ref[...] += dot_nn(flip(d_gate), w_a) + dot_nn(flip(d_lin), w_b)
    g_ref[:, 0] = dot_nn(d_gate, n2).astype(BF16).reshape(per, rows, wide)
    g_ref[:, 1] = dot_nn(d_lin, n2).astype(BF16).reshape(per, rows, wide)
    g_ref[:, 2] = dot_nn(gated, g_out).astype(BF16).reshape(per, rows, wide)

    @pl.when(step == pl.num_programs(0) - 1)
    def _():
        hidden = hid_ref[...].astype(F32)
        out_ref[...] = (hidden + mlp_ref[...].astype(BF16).astype(F32)).astype(BF16)
        d_n2 = dn_ref[...].astype(BF16).astype(F32)
        d_hid, gain_ref[...] = norm_back(hidden, d_n2, g2_ref[...])
        dh_ref[...] = (g_out.astype(F32) + d_hid.astype(BF16).astype(F32)).astype(BF16)


def attn_bwd_kernel(halo, tok, u_ref, dh_ref, w_ref, cos_ref, sin_ref, segc_ref, segr_ref,
                    qt_ref, kt_ref, vt_ref, ot_ref, lse_ref, g_ref, du_ref, bias_ref, acc_ref):
    own = pl.ds(halo, tok)
    step = pl.program_id(0)

    @pl.when(step == 0)
    def _():
        bias_ref[...] = jnp.where(segc_ref[...] == segr_ref[...], 0.0, NEG).astype(F32)

    heads, wide = w_ref.shape[0], w_ref.shape[3]
    d_hid = dh_ref[...]
    do_t = dot_nt(w_ref[:, 3].reshape(heads * HEAD_DIM, wide), d_hid).astype(BF16)
    o_t = ot_ref[...]
    g_ref[:, 3] = dot_nn(o_t, d_hid).astype(BF16).reshape(heads, HEAD_DIM, wide)
    cos_w, sin_w = cos_ref[...], sin_ref[...]
    cos_o, sin_o = cos_ref[:, halo:halo + tok], sin_ref[:, halo:halo + tok]
    dq_rows, dk_rows, dv_rows = [], [], []
    for head in range(heads):
        rows = slice(head * HEAD_DIM, (head + 1) * HEAD_DIM)
        q_t, k_t, v_t, d_o = qt_ref[rows, :], kt_ref[rows, :], vt_ref[rows, :], do_t[rows]
        score = dot_nn(flip(k_t), q_t) * S_SCALE + bias_ref[...]
        prob = jnp.exp2(score - lse_ref[0, head:head + 1, :])
        delta = jnp.sum(d_o.astype(F32) * o_t[rows].astype(F32), axis=0, keepdims=True)
        d_prob = dot_nn(flip(v_t), d_o).astype(BF16).astype(F32)
        d_score = (prob * (d_prob - delta)).astype(BF16)
        dv_rows.append(dot_nt(d_o, prob.astype(BF16)).astype(BF16))
        d_q = (dot_nn(k_t, d_score) * 0.125).astype(BF16).astype(F32)
        d_k = (dot_nt(q_t, d_score) * 0.125).astype(BF16).astype(F32)
        dq_rows += rope_back(d_q[:HALF], d_q[HALF:], cos_o, sin_o)
        dk_rows += rope_back(d_k[:HALF], d_k[HALF:], cos_w, sin_w)
    dq_t = jnp.concatenate(dq_rows, axis=0).astype(BF16)
    dk_t = jnp.concatenate(dk_rows, axis=0).astype(BF16)
    dv_t = jnp.concatenate(dv_rows, axis=0)
    u_win = u_ref[...]
    g_ref[:, 0] = dot_nn(dq_t, u_ref[own, :]).astype(BF16).reshape(heads, HEAD_DIM, wide)
    g_ref[:, 1] = dot_nn(dk_t, u_win).astype(BF16).reshape(heads, HEAD_DIM, wide)
    g_ref[:, 2] = dot_nn(dv_t, u_win).astype(BF16).reshape(heads, HEAD_DIM, wide)
    w_q = w_ref[:, 0].reshape(heads * HEAD_DIM, wide)
    w_kv = jnp.concatenate([w_ref[:, 1].reshape(heads * HEAD_DIM, wide), w_ref[:, 2].reshape(heads * HEAD_DIM, wide)], axis=0)
    d_kv = jnp.concatenate([flip(dk_t), flip(dv_t)], axis=1)
    term = dot_nn(d_kv, w_kv)

    @pl.when(step == 0)
    def _():
        acc_ref[...] = term

    @pl.when(step > 0)
    def _():
        acc_ref[...] += term

    acc_ref[own, :] += dot_nn(flip(dq_t), w_q)

    @pl.when(step == pl.num_programs(0) - 1)
    def _():
        du_ref[...] = acc_ref[...].astype(BF16)


def remote(src, dst, send_sem, recv_sem, where):
    return pltpu.make_async_remote_copy(src_ref=src, dst_ref=dst, send_sem=send_sem, recv_sem=recv_sem,
                                        device_id=where, device_id_type=pl.DeviceIdType.MESH)


def collect_kernel(cols, group, side, reach, x_ref, m_ref, w_ref, xw_ref, mw_ref, all_ref,
                   z_send, z_recv, c_send, c_recv, p_send, p_recv, h_send, h_recv, m_send, m_recv):
    col, me = lax.axis_index("dp"), lax.axis_index("tp")
    chips = group // 2
    chip, core = me // 2, me % 2
    tok = x_ref.shape[0]
    part_rows = w_ref.shape[0] // cols

    def column_at(pos):
        line, off = pos // side, pos % side
        return line * side + off + (line % 2) * (side - 1 - 2 * off)

    line, off = col // side, col % side
    pos = line * side + off + (line % 2) * (side - 1 - 2 * off)
    right_col, left_col = column_at((pos + 1) % cols), column_at((pos + cols - 1) % cols)
    partner = (col, chip * 2 + 1 - core)
    ahead, behind = (col, (me + 2) % group), (col, (me + group - 2) % group)

    peers = [(col, (me + by) % group) for by in range(1, reach + 1)]
    peers += [(col, (me + group - by) % group) for by in range(1, reach + 1)]
    if cols > 1:
        peers += [(right_col, me)]
    if cols > 2:
        peers += [(left_col, me)]
    barrier = pltpu.get_barrier_semaphore()
    for peer in peers:
        pl.semaphore_signal(barrier, inc=1, device_id=peer, device_id_type=pl.DeviceIdType.MESH)
    pl.semaphore_wait(barrier, len(peers))

    def part(pos_of):
        return pl.ds(pl.multiple_of((pos_of % cols) * part_rows, part_rows), part_rows)

    sends = []

    def send(src, dst, s_sem, r_sem, where):
        copy = remote(src, dst, s_sem, r_sem, where)
        copy.start()
        sends.append(copy)

    def arrived(dst, s_sem, r_sem):
        remote(dst, dst, s_sem, r_sem, partner).wait_recv()

    fwd_hops, back_hops = chips // 2, (chips - 1) // 2
    order = []
    for hop in range(1, fwd_hops + 1):
        order.append((1, hop))
        if hop <= back_hops:
            order.append((-1, hop))
    number = {key: slot for slot, key in enumerate(order)}

    own_part = w_ref.at[part(pos), :]
    send(own_part, all_ref.at[me, part(pos), :], z_send.at[number[1, 1]], z_recv.at[number[1, 1]], ahead)
    send(own_part, all_ref.at[me, part(pos), :], z_send.at[number[-1, 1]], z_recv.at[number[-1, 1]], behind)
    send(w_ref, all_ref.at[me], p_send.at[len(order), 0], p_recv.at[len(order), 0], partner)
    all_ref[me] = w_ref[...]
    xw_ref[pl.ds(reach * tok, tok), :] = x_ref[...]
    mw_ref[reach] = m_ref[...]

    def shard_of(slot):
        way, hop = order[slot]
        return ((chip + chips - way * hop) % chips) * 2 + core

    def hops_of(slot):
        right = (cols - 1 + slot % 2) // 2
        return right, cols - 1 - right

    for slot, (way, hop) in enumerate(order):
        place = all_ref.at[shard_of(slot), part(pos), :]
        arrived(place, z_send.at[slot], z_recv.at[slot])
        nxt = number.get((way, hop + 1))
        if nxt is not None:
            send(place, place, z_send.at[nxt], z_recv.at[nxt], ahead if way > 0 else behind)
        right, left = hops_of(slot)
        if right > 0:
            send(place, place, c_send.at[slot, cols - 1], c_recv.at[slot, cols - 1], (right_col, me))
        if left > 0:
            send(place, place, c_send.at[slot, 1], c_recv.at[slot, 1], (left_col, me))
        send(place, place, p_send.at[slot, 0], p_recv.at[slot, 0], partner)
    slots = []
    for slot in range(2 * reach + 1):
        by = reach - slot
        if by != 0:
            where = (col, (me + group + by) % group)
            send(x_ref, xw_ref.at[pl.ds(slot * tok, tok), :], h_send.at[slot], h_recv.at[slot], where)
            send(m_ref, mw_ref.at[slot], m_send.at[slot], m_recv.at[slot], where)
            slots.append(slot)
    for hop in range(1, cols // 2 + 1):
        for slot in range(len(order)):
            right, left = hops_of(slot)
            if hop <= right:
                place = all_ref.at[shard_of(slot), part(pos + cols - hop), :]
                arrived(place, c_send.at[slot, cols - hop], c_recv.at[slot, cols - hop])
                if hop < right:
                    send(place, place, c_send.at[slot, cols - hop - 1], c_recv.at[slot, cols - hop - 1], (right_col, me))
                send(place, place, p_send.at[slot, cols - hop], p_recv.at[slot, cols - hop], partner)
            if hop <= left:
                place = all_ref.at[shard_of(slot), part(pos + hop), :]
                arrived(place, c_send.at[slot, hop], c_recv.at[slot, hop])
                if hop < left:
                    send(place, place, c_send.at[slot, hop + 1], c_recv.at[slot, hop + 1], (left_col, me))
                send(place, place, p_send.at[slot, hop], p_recv.at[slot, hop], partner)
    other = chip * 2 + 1 - core
    for slot in range(len(order)):
        shard = shard_of(slot) + 1 - 2 * core
        for away in range(cols):
            arrived(all_ref.at[shard, part(pos + away), :], p_send.at[slot, away], p_recv.at[slot, away])
    arrived(all_ref.at[other], p_send.at[len(order), 0], p_recv.at[len(order), 0])
    for slot in slots:
        arrived(xw_ref.at[pl.ds(slot * tok, tok), :], h_send.at[slot], h_recv.at[slot])
        arrived(mw_ref.at[slot], m_send.at[slot], m_recv.at[slot])
    for copy in sends:
        copy.wait_send()


def collect(x_in, marks, w_rows, cols, group, reach):
    tok, dim = x_in.shape
    rows = w_rows.shape[0]
    side = math.isqrt(cols)
    side = side if side * side == cols else 1
    vmem = pl.BlockSpec(memory_space=pltpu.VMEM)
    shards = group // 2
    dma = pltpu.SemaphoreType.DMA
    window = (2 * reach + 1) * tok
    return pl.pallas_call(
        lambda *refs: collect_kernel(cols, group, side, reach, *refs),
        in_specs=[vmem] * 3,
        out_specs=[vmem] * 3,
        out_shape=[jax.ShapeDtypeStruct((window, dim), BF16),
                   jax.ShapeDtypeStruct((2 * reach + 1,) + marks.shape, marks.dtype),
                   jax.ShapeDtypeStruct((group, rows, dim), BF16)],
        scratch_shapes=[dma((shards,)), dma((shards,)), dma((shards, cols)), dma((shards, cols)),
                        dma((shards, cols)), dma((shards, cols)), dma((2 * reach + 1,)), dma((2 * reach + 1,)),
                        dma((2 * reach + 1,)), dma((2 * reach + 1,))],
        compiler_params=pltpu.CompilerParams(collective_id=0, has_side_effects=True, vmem_limit_bytes=40 * 1024 * 1024),
        cost_estimate=pl.CostEstimate(flops=60_000_000_000, bytes_accessed=20_000_000, transcendentals=0),
        name="collect",
    )(x_in, marks, w_rows)


def norm_back(values, d_normed, gain):
    centered = values - jnp.mean(values, axis=-1, keepdims=True)
    rstd = lax.rsqrt(jnp.mean(centered * centered, axis=-1, keepdims=True) + 1e-5)
    unit = centered * rstd
    d_unit = d_normed * gain
    d_val = rstd * (d_unit - jnp.mean(d_unit, axis=-1, keepdims=True)
                    - unit * jnp.mean(d_unit * unit, axis=-1, keepdims=True))
    return d_val, jnp.sum(d_normed * unit, axis=0, keepdims=True)


def reduce_kernel(group, reach, g_ref, du_ref, x_ref, dh_ref, g1_ref, gain2_ref, sum_ref, gx_ref, gains_ref,
                  ring_ref, back_ref, term_ref, r_send, r_recv, h_send, h_recv, t_send, t_recv):
    col, me = lax.axis_index("dp"), lax.axis_index("tp")
    tok = x_ref.shape[0]
    piece = g_ref.shape[1] // (2 * STREAMS)
    up, down = (col, (me + 1) % group), (col, (me + group - 1) % group)
    levels = group.bit_length() - 1

    def flipped(level):
        span = 2 ** level
        return (col, me + span - 2 * span * ((me // span) % 2))

    peers = [(col, (me + by) % group) for by in range(1, reach + 1)]
    peers += [(col, (me + group - by) % group) for by in range(1, reach + 1)]
    peers += [flipped(level) for level in range(levels)]
    barrier = pltpu.get_barrier_semaphore()
    for peer in peers:
        pl.semaphore_signal(barrier, inc=1, device_id=peer, device_id_type=pl.DeviceIdType.MESH)
    pl.semaphore_wait(barrier, len(peers))

    lanes = [(way, part) for part in range(STREAMS) for way in range(2)]

    def rows_of(way, part):
        return pl.ds((way * STREAMS + part) * piece, piece)

    def shard_at(way, hop):
        return (me + 2 * group - 1 - hop) % group if way == 0 else (me + 1 + hop) % group

    for way, part in lanes:
        remote(g_ref.at[shard_at(way, 0), rows_of(way, part), :], ring_ref.at[way, part, 0],
               r_send.at[way, part, 0], r_recv.at[way, part, 0], down if way else up).start()

    slots = [slot for slot in range(2 * reach + 1) if slot != reach]
    sends = []
    for slot in slots:
        by = reach - slot
        copy = remote(du_ref.at[pl.ds(slot * tok, tok), :], back_ref.at[slot], h_send.at[slot], h_recv.at[slot],
                      (col, (me + group - by) % group))
        copy.start()
        sends.append(copy)

    def ring_step(hop, carry):
        for way, part in lanes:
            slot = ring_ref.at[way, part, hop - 1]
            remote(slot, slot, r_send.at[way, part, hop - 1], r_recv.at[way, part, hop - 1], up).wait_recv()
            mine = g_ref[shard_at(way, hop), rows_of(way, part), :]
            slot[...] = (slot[...].astype(F32) + mine.astype(F32)).astype(BF16)
            remote(slot, ring_ref.at[way, part, hop], r_send.at[way, part, hop], r_recv.at[way, part, hop],
                   down if way else up).start()
        return carry

    middle = group // 2
    lax.fori_loop(1, middle, ring_step, 0)

    total = du_ref[pl.ds(reach * tok, tok), :].astype(F32)
    for slot in slots:
        place = back_ref.at[slot]
        remote(place, place, h_send.at[slot], h_recv.at[slot], up).wait_recv()
        total = total + place[...].astype(F32)
    d_val, g_gain1 = norm_back(x_ref[...].astype(F32), total.astype(BF16).astype(F32), g1_ref[...])
    gx_ref[...] = (dh_ref[...].astype(F32) + d_val.astype(BF16).astype(F32)).astype(BF16)
    term_ref[0, 0] = jnp.zeros(term_ref.shape[2:], F32)
    term_ref[0, 0, 0:1, :] = g_gain1
    term_ref[0, 0, 1:2, :] = gain2_ref[...]
    for level in range(levels):
        ring_step(middle + level, 0)
        copy = remote(term_ref.at[level, 0], term_ref.at[level, 1], t_send.at[level], t_recv.at[level], flipped(level))
        copy.start()
        sends.append(copy)
        copy.wait_recv()
        both = term_ref[level, 0] + term_ref[level, 1]
        if level + 1 < levels:
            term_ref[level + 1, 0] = both
        else:
            gains_ref[...] = both[0:2]
    lax.fori_loop(middle + levels, group - 1, ring_step, 0)

    for way, part in lanes:
        slot = ring_ref.at[way, part, group - 2]
        remote(slot, slot, r_send.at[way, part, group - 2], r_recv.at[way, part, group - 2], up).wait_recv()
        sum_ref[rows_of(way, part), :] = slot[...].astype(F32) + g_ref[me, rows_of(way, part), :].astype(F32)
    for copy in sends:
        copy.wait_send()

    def drain(hop, carry):
        for way, part in lanes:
            slot = ring_ref.at[way, part, hop]
            remote(slot, slot, r_send.at[way, part, hop], r_recv.at[way, part, hop], up).wait_send()
        return carry

    lax.fori_loop(0, group - 1, drain, 0)


def reduce_rows(g_att, du_win, x_in, d_hidden, gain1, g_gain2, reach):
    group, rows, dim = g_att.shape
    tok = x_in.shape[0]
    levels = group.bit_length() - 1
    piece = rows // (2 * STREAMS)
    vmem = pl.BlockSpec(memory_space=pltpu.VMEM)
    dma = pltpu.SemaphoreType.DMA
    return pl.pallas_call(
        lambda *refs: reduce_kernel(group, reach, *refs),
        in_specs=[vmem] * 6,
        out_specs=[vmem] * 3,
        out_shape=[jax.ShapeDtypeStruct((rows, dim), F32), jax.ShapeDtypeStruct((tok, dim), BF16),
                   jax.ShapeDtypeStruct((2, dim), F32)],
        scratch_shapes=[pltpu.VMEM((2, STREAMS, group - 1, piece, dim), BF16),
                        pltpu.VMEM((2 * reach + 1, tok, dim), BF16),
                        pltpu.VMEM((levels, 2, 8, dim), F32),
                        dma((2, STREAMS, group - 1)), dma((2, STREAMS, group - 1)),
                        dma((2 * reach + 1,)), dma((2 * reach + 1,)), dma((levels,)), dma((levels,))],
        compiler_params=pltpu.CompilerParams(collective_id=1, has_side_effects=True, vmem_limit_bytes=48 * 1024 * 1024),
        cost_estimate=pl.CostEstimate(flops=60_000_000_000, bytes_accessed=20_000_000, transcendentals=0),
        name="reduce",
    )(g_att, du_win, x_in, d_hidden, gain1, g_gain2)


def whole(shape):
    return pl.BlockSpec(shape, lambda i: (0,) * len(shape))


def attn_forward(x_win, gain1, gain2, w_att, cos_t, sin_t, seg_col, seg_row, tok, heads):
    win, dim = x_win.shape
    halo = (win - tok) // 2
    per = math.gcd(heads, HEADS_STEP)
    steps = heads // per
    feat = per * HEAD_DIM
    return pl.pallas_call(
        lambda *refs: attn_fwd_kernel(halo, tok, *refs),
        grid=(steps,),
        in_specs=[whole((win, dim)), whole((1, dim)), whole((1, dim)),
                  pl.BlockSpec((per, 4, HEAD_DIM, dim), lambda i: (i, 0, 0, 0)),
                  whole((HALF, win)), whole((HALF, win)), whole((win, 1)), whole((1, tok))],
        out_specs=[whole((win, dim)),
                   pl.BlockSpec((feat, tok), lambda i: (i, 0)),
                   pl.BlockSpec((feat, win), lambda i: (i, 0)),
                   pl.BlockSpec((feat, win), lambda i: (i, 0)),
                   pl.BlockSpec((feat, tok), lambda i: (i, 0)),
                   pl.BlockSpec((1, per, tok), lambda i: (i, 0, 0)),
                   whole((tok, dim)), whole((tok, dim))],
        out_shape=[jax.ShapeDtypeStruct((win, dim), BF16),
                   jax.ShapeDtypeStruct((heads * HEAD_DIM, tok), BF16),
                   jax.ShapeDtypeStruct((heads * HEAD_DIM, win), BF16),
                   jax.ShapeDtypeStruct((heads * HEAD_DIM, win), BF16),
                   jax.ShapeDtypeStruct((heads * HEAD_DIM, tok), BF16),
                   jax.ShapeDtypeStruct((steps, per, tok), F32),
                   jax.ShapeDtypeStruct((tok, dim), BF16),
                   jax.ShapeDtypeStruct((tok, dim), BF16)],
        scratch_shapes=[pltpu.VMEM((win, tok), F32), pltpu.VMEM((tok, dim), F32)],
        compiler_params=pltpu.CompilerParams(dimension_semantics=("arbitrary",), vmem_limit_bytes=40 * 1024 * 1024),
        cost_estimate=pl.CostEstimate(flops=20_000_000_000, bytes_accessed=20_000_000, transcendentals=5_000_000),
        name="attn_fwd",
    )(x_win, gain1, gain2, w_att, cos_t, sin_t, seg_col, seg_row)


def mlp(normed2, hidden, grad_out, gain2, w_first, w_rest, rows):
    tok, dim = normed2.shape
    shards = w_rest.shape[0]
    parts = 3
    per = math.gcd(shards, MLP_SHARDS)
    block = pl.BlockSpec((per, parts, rows, dim), lambda i: (i, 0, 0, 0))
    return pl.pallas_call(
        mlp_kernel,
        grid=(shards // per,),
        in_specs=[whole((tok, dim)), whole((tok, dim)), whole((tok, dim)), whole((1, dim)),
                  pl.BlockSpec((per, EXTRA // HEAD_DIM, HEAD_DIM, dim), lambda i: (i, w_first.shape[1] * HEAD_DIM // EXTRA - 1, 0, 0)),
                  pl.BlockSpec((per, w_rest.shape[1], dim), lambda i: (i, 0, 0))],
        out_specs=[block, whole((tok, dim)), whole((tok, dim)), whole((1, dim))],
        out_shape=[jax.ShapeDtypeStruct((shards, parts, rows, dim), BF16),
                   jax.ShapeDtypeStruct((tok, dim), BF16),
                   jax.ShapeDtypeStruct((tok, dim), BF16),
                   jax.ShapeDtypeStruct((1, dim), F32)],
        scratch_shapes=[pltpu.VMEM((tok, dim), F32), pltpu.VMEM((tok, dim), F32)],
        compiler_params=pltpu.CompilerParams(dimension_semantics=("arbitrary",), vmem_limit_bytes=40 * 1024 * 1024),
        cost_estimate=pl.CostEstimate(flops=20_000_000_000, bytes_accessed=35_000_000, transcendentals=1_500_000),
        name="mlp",
    )(normed2, hidden, grad_out, gain2, w_first, w_rest)


def attn_backward(u_win, d_hid, w_att, cos_t, sin_t, seg_col, seg_row, q_t, k_t, v_t, o_t, lse, heads):
    win, dim = u_win.shape
    tok = d_hid.shape[0]
    halo = (win - tok) // 2
    per = math.gcd(heads, HEADS_STEP)
    steps = heads // per
    feat = per * HEAD_DIM
    return pl.pallas_call(
        lambda *refs: attn_bwd_kernel(halo, tok, *refs),
        grid=(steps,),
        in_specs=[whole((win, dim)), whole((tok, dim)),
                  pl.BlockSpec((per, 4, HEAD_DIM, dim), lambda i: (i, 0, 0, 0)),
                  whole((HALF, win)), whole((HALF, win)), whole((win, 1)), whole((1, tok)),
                  pl.BlockSpec((feat, tok), lambda i: (i, 0)),
                  pl.BlockSpec((feat, win), lambda i: (i, 0)),
                  pl.BlockSpec((feat, win), lambda i: (i, 0)),
                  pl.BlockSpec((feat, tok), lambda i: (i, 0)),
                  pl.BlockSpec((1, per, tok), lambda i: (i, 0, 0))],
        out_specs=[pl.BlockSpec((per, 4, HEAD_DIM, dim), lambda i: (i, 0, 0, 0)), whole((win, dim))],
        out_shape=[jax.ShapeDtypeStruct((heads, 4, HEAD_DIM, dim), BF16),
                   jax.ShapeDtypeStruct((win, dim), BF16)],
        scratch_shapes=[pltpu.VMEM((win, tok), F32), pltpu.VMEM((win, dim), F32)],
        compiler_params=pltpu.CompilerParams(dimension_semantics=("arbitrary",), vmem_limit_bytes=48 * 1024 * 1024),
        cost_estimate=pl.CostEstimate(flops=40_000_000_000, bytes_accessed=30_000_000, transcendentals=5_000_000),
        name="attn_bwd",
    )(u_win, d_hid, w_att, cos_t, sin_t, seg_col, seg_row, q_t, k_t, v_t, o_t, lse)


def solution(mesh):
    tok_spec = P(('dp', 'tp'), None)
    seq_spec = P(('dp', 'tp'))
    in_specs = (tok_spec, seq_spec, seq_spec, P(None), P(None, None, 'tp'), P('tp', None),
                P(None), P(None, None, 'tp'), P('tp', None), tok_spec)
    out_specs = (tok_spec, tok_spec, P('dp'), P('dp', None, 'tp'), P(('dp', 'tp'), None),
                 P('dp'), P('dp', None, 'tp'), P(('dp', 'tp'), None))
    group = mesh.shape['tp']
    cols = mesh.shape['dp']

    def gather_rows(shard_rows):
        return lax.all_gather(shard_rows, 'tp', axis=0, tiled=True)

    def scatter_rows(part_sum):
        return lax.psum_scatter(part_sum, 'tp', scatter_dimension=0, tiled=True)

    def device_step(x_in, doc_ids, doc_pos, gamma1, w_qkv, w_out, gamma2, w_in, w_down, grad_out):
        tok, dim = x_in.shape
        heads_loc = w_qkv.shape[2] // HEAD_DIM
        ff_loc = w_in.shape[2]
        ff_pad = -(-ff_loc // FF_ALIGN) * FF_ALIGN
        reach = -(-MAX_DOC // tok)
        qkv_rows = jnp.transpose(w_qkv.reshape(dim, 3, heads_loc, HEAD_DIM), (2, 1, 3, 0))
        out_rows = w_out.reshape(heads_loc, 1, HEAD_DIM, dim)
        att_rows = jnp.concatenate([qkv_rows, out_rows], axis=1)
        mlp_rows = jnp.concatenate([jnp.transpose(w_in, (1, 2, 0)), w_down[None]], axis=0)
        mlp_rows = jnp.pad(mlp_rows, ((0, 0), (0, ff_pad - ff_loc), (0, 0))).reshape(3 * ff_pad, dim)
        first_rows = jnp.concatenate([att_rows.reshape(-1, dim), mlp_rows[:EXTRA]], axis=0)
        x_win, marks, w_first = collect(x_in, jnp.stack([doc_ids, doc_pos]), first_rows, cols, group, reach)
        w_rest = gather_rows(mlp_rows[EXTRA:]).reshape(group, 3 * ff_pad - EXTRA, dim)
        w_first = w_first.reshape(group, -1, HEAD_DIM, dim)
        seg_row, seg_col = doc_ids[None, :], marks[:, 0].reshape(-1, 1)
        inv_freq = 160000.0 ** (-jnp.arange(HALF, dtype=F32) / HALF)
        angle = marks[:, 1].reshape(1, -1).astype(F32) * inv_freq[:, None]
        cos_t, sin_t = jnp.cos(angle), jnp.sin(angle)


        gain1 = gamma1.astype(F32)[None, :]
        gain2 = gamma2.astype(F32)[None, :]
        u_win, q_t, k_t, v_t, o_t, lse, hidden, normed2 = attn_forward(
            x_win, gain1, gain2, w_first, cos_t, sin_t, seg_col, seg_row, tok, group * heads_loc)
        g_mlp, layer_out, d_hidden, g_gain2 = mlp(normed2, hidden, grad_out, gain2, w_first, w_rest, ff_pad)
        g_mlp = scatter_rows(g_mlp.reshape(group * 3 * ff_pad, dim))
        g_att, du_win = attn_backward(u_win, d_hidden, w_first, cos_t, sin_t, seg_col, seg_row,
                                      q_t, k_t, v_t, o_t, lse, group * heads_loc)
        g_att, grad_x, gains = reduce_rows(g_att.reshape(group, heads_loc * 4 * HEAD_DIM, dim), du_win, x_in,
                                           d_hidden, gain1, g_gain2, reach)

        g_att = g_att.reshape(heads_loc, 4, HEAD_DIM, dim)
        g_qkv = jnp.transpose(g_att[:, :3], (3, 1, 0, 2)).reshape(dim, 3, heads_loc * HEAD_DIM)
        g_out = g_att[:, 3].reshape(heads_loc * HEAD_DIM, dim)
        g_mlp = g_mlp.reshape(3, ff_pad, dim)[:, :ff_loc].astype(F32)
        g_in = jnp.transpose(g_mlp[:2], (2, 0, 1))
        return (layer_out, grad_x, gains[0], g_qkv, g_out, gains[1], g_in, g_mlp[2])

    return jax.shard_map(device_step, mesh=mesh, in_specs=in_specs, out_specs=out_specs, check_vma=False)
```

```python
import math
import jax
import jax.numpy as jnp
from jax import lax
from jax.experimental import pallas as pl
from jax.experimental.pallas import tpu as pltpu
from jax.sharding import PartitionSpec as P

MAX_DOC = 512
HEAD_DIM = 64
HALF = HEAD_DIM // 2
VMEM_GRANT = 60 * 2 ** 20
FF_ALIGN = 8
MLP_SHARDS = 4
HEADS_STEP = 4
EXTRA = 256
STREAMS = 2
LOG2E = 1.4426950408889634
S_SCALE = 0.125 * LOG2E
NEG = -1e30
SQRT_HALF = 0.7071067811865476
INV_SQRT_2PI = 0.3989422804014327
F32 = jnp.float32
BF16 = jnp.bfloat16
COST = pl.CostEstimate(flops=30_000_000_000, bytes_accessed=30_000_000, transcendentals=5_000_000)


def layer_norm(values, gain):
    vals32 = values.astype(F32)
    mean_val = jnp.mean(vals32, axis=-1, keepdims=True)
    centered = vals32 - mean_val
    var_val = jnp.mean(centered * centered, axis=-1, keepdims=True)
    return (centered * lax.rsqrt(var_val + 1e-5) * gain).astype(BF16)


def dot_nn(a, b):
    return lax.dot_general(a, b, (((1,), (0,)), ((), ())), preferred_element_type=F32)


def dot_nt(a, b):
    return lax.dot_general(a, b, (((1,), (1,)), ((), ())), preferred_element_type=F32)


def dot_tn(a, b):
    return lax.dot_general(a, b, (((0,), (0,)), ((), ())), preferred_element_type=F32)


def flip(vals):
    return vals.astype(F32).T.astype(BF16)


def rope_fwd(vals_t, cos_t, sin_t):
    rows = []
    for head in range(vals_t.shape[0] // HEAD_DIM):
        lo = vals_t[head * HEAD_DIM: head * HEAD_DIM + HALF]
        hi = vals_t[head * HEAD_DIM + HALF: (head + 1) * HEAD_DIM]
        rows += [lo * cos_t - hi * sin_t, hi * cos_t + lo * sin_t]
    return jnp.concatenate(rows, axis=0)


def rope_back(lo, hi, cos_t, sin_t):
    return [lo * cos_t + hi * sin_t, hi * cos_t - lo * sin_t]


def attn_fwd_kernel(halo, tok, x_ref, g1_ref, g2_ref, w_ref, cos_ref, sin_ref, segc_ref, segr_ref,
                    u_ref, qt_ref, kt_ref, vt_ref, ot_ref, lse_ref, hid_ref, n2_ref, bias_ref, att_ref):
    own = pl.ds(halo, tok)
    step = pl.program_id(0)

    @pl.when(step == 0)
    def _():
        u_ref[...] = layer_norm(x_ref[...], g1_ref[...])
        bias_ref[...] = jnp.where(segc_ref[...] == segr_ref[...], 0.0, NEG).astype(F32)
        att_ref[...] = jnp.zeros_like(att_ref)

    heads, wide = w_ref.shape[0], w_ref.shape[3]
    w_q, w_k, w_v, w_o = [w_ref[:, part].reshape(heads * HEAD_DIM, wide) for part in range(4)]
    u_win = u_ref[...]
    u_own = u_ref[own, :]
    q_raw = dot_nt(w_q, u_own).astype(BF16).astype(F32)
    k_raw = dot_nt(w_k, u_win).astype(BF16).astype(F32)
    v_t = dot_nt(w_v, u_win).astype(BF16)
    q_t = rope_fwd(q_raw, cos_ref[:, halo:halo + tok], sin_ref[:, halo:halo + tok]).astype(BF16)
    k_t = rope_fwd(k_raw, cos_ref[...], sin_ref[...]).astype(BF16)
    qt_ref[...] = q_t
    kt_ref[...] = k_t
    vt_ref[...] = v_t
    for head in range(heads):
        rows = slice(head * HEAD_DIM, (head + 1) * HEAD_DIM)
        score = dot_nn(flip(k_t[rows]), q_t[rows]) * S_SCALE + bias_ref[...]
        top = jnp.max(score, axis=0, keepdims=True)
        expd = jnp.exp2(score - top)
        total = jnp.sum(expd, axis=0, keepdims=True)
        prob = (expd * (1.0 / total)).astype(BF16)
        ot_ref[rows, :] = dot_nn(v_t[rows], prob).astype(BF16)
        lse_ref[0, head:head + 1, :] = top + jnp.log2(total)
    att_ref[...] += dot_nn(flip(ot_ref[...]), w_o)

    @pl.when(step == pl.num_programs(0) - 1)
    def _():
        hidden = (x_ref[own, :].astype(F32) + att_ref[...].astype(BF16).astype(F32)).astype(BF16)
        hid_ref[...] = hidden
        n2_ref[...] = layer_norm(hidden, g2_ref[...])


def mlp_kernel(n2_ref, hid_ref, go_ref, g2_ref, we_ref, wr_ref, g_ref, out_ref, dh_ref, gain_ref, mlp_ref, dn_ref):
    step = pl.program_id(0)

    @pl.when(step == 0)
    def _():
        mlp_ref[...] = jnp.zeros_like(mlp_ref)
        dn_ref[...] = jnp.zeros_like(dn_ref)

    n2 = n2_ref[...]
    g_out = go_ref[...]
    per, _, rows, wide = g_ref.shape
    lead = we_ref.shape[1] * we_ref.shape[2]
    first, rest = we_ref[...].reshape(per, lead, wide), wr_ref[...]
    w_a = first[:, :rows].reshape(per * rows, wide)
    w_b = jnp.concatenate([first[:, rows:], rest[:, :2 * rows - lead]], axis=1).reshape(per * rows, wide)
    w_d = rest[:, 2 * rows - lead:].reshape(per * rows, wide)
    gate = dot_nt(w_a, n2).astype(BF16).astype(F32)
    lin = dot_nt(w_b, n2).astype(BF16).astype(F32)
    cdf = 0.5 * (1.0 + lax.erf(gate * SQRT_HALF))
    act = gate * cdf
    gated = (act * lin).astype(BF16)
    d_gated = dot_nt(w_d, g_out).astype(BF16).astype(F32)
    slope = cdf + gate * (jnp.exp2(gate * gate * (-0.5 * LOG2E)) * INV_SQRT_2PI)
    d_gate = (d_gated * lin * slope).astype(BF16)
    d_lin = (d_gated * act).astype(BF16)
    mlp_ref[...] += dot_nn(flip(gated), w_d)
    dn_ref[...] += dot_nn(flip(d_gate), w_a) + dot_nn(flip(d_lin), w_b)
    g_ref[:, 0] = dot_nn(d_gate, n2).astype(BF16).reshape(per, rows, wide)
    g_ref[:, 1] = dot_nn(d_lin, n2).astype(BF16).reshape(per, rows, wide)
    g_ref[:, 2] = dot_nn(gated, g_out).astype(BF16).reshape(per, rows, wide)

    @pl.when(step == pl.num_programs(0) - 1)
    def _():
        hidden = hid_ref[...].astype(F32)
        out_ref[...] = (hidden + mlp_ref[...].astype(BF16).astype(F32)).astype(BF16)
        d_n2 = dn_ref[...].astype(BF16).astype(F32)
        d_hid, gain_ref[...] = norm_back(hidden, d_n2, g2_ref[...])
        dh_ref[...] = (g_out.astype(F32) + d_hid.astype(BF16).astype(F32)).astype(BF16)


def attn_bwd_kernel(halo, tok, u_ref, dh_ref, w_ref, cos_ref, sin_ref, segc_ref, segr_ref,
                    qt_ref, kt_ref, vt_ref, ot_ref, lse_ref, g_ref, du_ref, bias_ref, acc_ref):
    own = pl.ds(halo, tok)
    step = pl.program_id(0)

    @pl.when(step == 0)
    def _():
        bias_ref[...] = jnp.where(segc_ref[...] == segr_ref[...], 0.0, NEG).astype(F32)

    heads, wide = w_ref.shape[0], w_ref.shape[3]
    d_hid = dh_ref[...]
    do_t = dot_nt(w_ref[:, 3].reshape(heads * HEAD_DIM, wide), d_hid).astype(BF16)
    o_t = ot_ref[...]
    g_ref[:, 3] = dot_nn(o_t, d_hid).astype(BF16).reshape(heads, HEAD_DIM, wide)
    cos_w, sin_w = cos_ref[...], sin_ref[...]
    cos_o, sin_o = cos_ref[:, halo:halo + tok], sin_ref[:, halo:halo + tok]
    dq_rows, dk_rows, dv_rows = [], [], []
    for head in range(heads):
        rows = slice(head * HEAD_DIM, (head + 1) * HEAD_DIM)
        q_t, k_t, v_t, d_o = qt_ref[rows, :], kt_ref[rows, :], vt_ref[rows, :], do_t[rows]
        score = dot_nn(flip(k_t), q_t) * S_SCALE + bias_ref[...]
        prob = jnp.exp2(score - lse_ref[0, head:head + 1, :])
        delta = jnp.sum(d_o.astype(F32) * o_t[rows].astype(F32), axis=0, keepdims=True)
        d_prob = dot_nn(flip(v_t), d_o).astype(BF16).astype(F32)
        d_score = (prob * (d_prob - delta)).astype(BF16)
        dv_rows.append(dot_nt(d_o, prob.astype(BF16)).astype(BF16))
        d_q = (dot_nn(k_t, d_score) * 0.125).astype(BF16).astype(F32)
        d_k = (dot_nt(q_t, d_score) * 0.125).astype(BF16).astype(F32)
        dq_rows += rope_back(d_q[:HALF], d_q[HALF:], cos_o, sin_o)
        dk_rows += rope_back(d_k[:HALF], d_k[HALF:], cos_w, sin_w)
    dq_t = jnp.concatenate(dq_rows, axis=0).astype(BF16)
    dk_t = jnp.concatenate(dk_rows, axis=0).astype(BF16)
    dv_t = jnp.concatenate(dv_rows, axis=0)
    u_win = u_ref[...]
    g_ref[:, 0] = dot_nn(dq_t, u_ref[own, :]).astype(BF16).reshape(heads, HEAD_DIM, wide)
    g_ref[:, 1] = dot_nn(dk_t, u_win).astype(BF16).reshape(heads, HEAD_DIM, wide)
    g_ref[:, 2] = dot_nn(dv_t, u_win).astype(BF16).reshape(heads, HEAD_DIM, wide)
    w_q = w_ref[:, 0].reshape(heads * HEAD_DIM, wide)
    w_kv = jnp.concatenate([w_ref[:, 1].reshape(heads * HEAD_DIM, wide), w_ref[:, 2].reshape(heads * HEAD_DIM, wide)], axis=0)
    d_kv = jnp.concatenate([flip(dk_t), flip(dv_t)], axis=1)
    term = dot_nn(d_kv, w_kv)

    @pl.when(step == 0)
    def _():
        acc_ref[...] = term

    @pl.when(step > 0)
    def _():
        acc_ref[...] += term

    acc_ref[own, :] += dot_nn(flip(dq_t), w_q)

    @pl.when(step == pl.num_programs(0) - 1)
    def _():
        du_ref[...] = acc_ref[...].astype(BF16)


def remote(src, dst, send_sem, recv_sem, where):
    return pltpu.make_async_remote_copy(src_ref=src, dst_ref=dst, send_sem=send_sem, recv_sem=recv_sem,
                                        device_id=where, device_id_type=pl.DeviceIdType.MESH)


def collect_kernel(cols, group, side, reach, x_ref, m_ref, w_ref, xw_ref, mw_ref, out_ref, all_ref,
                   z_send, z_recv, c_send, c_recv, p_send, p_recv, h_send, h_recv, m_send, m_recv, k_sem):
    col, me = lax.axis_index("dp"), lax.axis_index("tp")
    chips = group // 2
    chip, core = me // 2, me % 2
    tok = x_ref.shape[0]
    part_rows = w_ref.shape[0] // cols

    def column_at(pos):
        line, off = pos // side, pos % side
        return line * side + off + (line % 2) * (side - 1 - 2 * off)

    line, off = col // side, col % side
    pos = line * side + off + (line % 2) * (side - 1 - 2 * off)
    right_col, left_col = column_at((pos + 1) % cols), column_at((pos + cols - 1) % cols)
    partner = (col, chip * 2 + 1 - core)
    ahead, behind = (col, (me + 2) % group), (col, (me + group - 2) % group)

    peers = [(col, (me + by) % group) for by in range(1, reach + 1)]
    peers += [(col, (me + group - by) % group) for by in range(1, reach + 1)]
    if cols > 1:
        peers += [(right_col, me)]
    if cols > 2:
        peers += [(left_col, me)]
    barrier = pltpu.get_barrier_semaphore()
    for peer in peers:
        pl.semaphore_signal(barrier, inc=1, device_id=peer, device_id_type=pl.DeviceIdType.MESH)
    pl.semaphore_wait(barrier, len(peers))

    def part(pos_of):
        return pl.ds(pl.multiple_of((pos_of % cols) * part_rows, part_rows), part_rows)

    sends = []

    def send(src, dst, s_sem, r_sem, where):
        copy = remote(src, dst, s_sem, r_sem, where)
        copy.start()
        sends.append(copy)

    def arrived(dst, s_sem, r_sem):
        remote(dst, dst, s_sem, r_sem, partner).wait_recv()

    kept = []

    def keep(src, dst, sem):
        copy = pltpu.make_async_copy(src, dst, sem)
        copy.start()
        kept.append(copy)

    fwd_hops, back_hops = chips // 2, (chips - 1) // 2
    order = []
    for hop in range(1, fwd_hops + 1):
        order.append((1, hop))
        if hop <= back_hops:
            order.append((-1, hop))
    number = {key: slot for slot, key in enumerate(order)}

    own_part = w_ref.at[part(pos), :]
    send(own_part, all_ref.at[me, part(pos), :], z_send.at[number[1, 1]], z_recv.at[number[1, 1]], ahead)
    send(own_part, all_ref.at[me, part(pos), :], z_send.at[number[-1, 1]], z_recv.at[number[-1, 1]], behind)
    send(w_ref, all_ref.at[me], p_send.at[len(order), 0], p_recv.at[len(order), 0], partner)
    keep(w_ref, out_ref.at[me], k_sem.at[len(order), 0])
    xw_ref[pl.ds(reach * tok, tok), :] = x_ref[...]
    mw_ref[reach] = m_ref[...]

    def shard_of(slot):
        way, hop = order[slot]
        return ((chip + chips - way * hop) % chips) * 2 + core

    def hops_of(slot):
        right = (cols - 1 + slot % 2) // 2
        return right, cols - 1 - right

    for slot, (way, hop) in enumerate(order):
        place = all_ref.at[shard_of(slot), part(pos), :]
        arrived(place, z_send.at[slot], z_recv.at[slot])
        keep(place, out_ref.at[shard_of(slot), part(pos), :], k_sem.at[slot, 0])
        nxt = number.get((way, hop + 1))
        if nxt is not None:
            send(place, place, z_send.at[nxt], z_recv.at[nxt], ahead if way > 0 else behind)
        right, left = hops_of(slot)
        if right > 0:
            send(place, place, c_send.at[slot, cols - 1], c_recv.at[slot, cols - 1], (right_col, me))
        if left > 0:
            send(place, place, c_send.at[slot, 1], c_recv.at[slot, 1], (left_col, me))
        send(place, place, p_send.at[slot, 0], p_recv.at[slot, 0], partner)
    def window_slot(slot):
        return xw_ref.at[pl.ds(pl.multiple_of(slot * tok, tok), tok), :]

    def halo_send(src, marks, slot, where):
        send(src, window_slot(slot), h_send.at[slot], h_recv.at[slot], where)
        send(marks, mw_ref.at[slot], m_send.at[slot], m_recv.at[slot], where)

    def halo_arrived(slot):
        arrived(window_slot(slot), h_send.at[slot], h_recv.at[slot])
        arrived(mw_ref.at[slot], m_send.at[slot], m_recv.at[slot])

    halo_send(x_ref, m_ref, 0, ahead)
    halo_send(x_ref, m_ref, 4, behind)
    halo_send(x_ref, m_ref, 1 + 2 * core, partner)
    for hop in range(1, cols // 2 + 1):
        for slot in range(len(order)):
            right, left = hops_of(slot)
            if hop <= right:
                place = all_ref.at[shard_of(slot), part(pos + cols - hop), :]
                arrived(place, c_send.at[slot, cols - hop], c_recv.at[slot, cols - hop])
                keep(place, out_ref.at[shard_of(slot), part(pos + cols - hop), :], k_sem.at[slot, cols - hop])
                if hop < right:
                    send(place, place, c_send.at[slot, cols - hop - 1], c_recv.at[slot, cols - hop - 1], (right_col, me))
                send(place, place, p_send.at[slot, cols - hop], p_recv.at[slot, cols - hop], partner)
            if hop <= left:
                place = all_ref.at[shard_of(slot), part(pos + hop), :]
                arrived(place, c_send.at[slot, hop], c_recv.at[slot, hop])
                keep(place, out_ref.at[shard_of(slot), part(pos + hop), :], k_sem.at[slot, hop])
                if hop < left:
                    send(place, place, c_send.at[slot, hop + 1], c_recv.at[slot, hop + 1], (left_col, me))
                send(place, place, p_send.at[slot, hop], p_recv.at[slot, hop], partner)
    other = chip * 2 + 1 - core
    for slot in range(len(order)):
        shard = shard_of(slot) + 1 - 2 * core
        for away in range(cols):
            place = all_ref.at[shard, part(pos + away), :]
            arrived(place, p_send.at[slot, away], p_recv.at[slot, away])
            keep(place, out_ref.at[shard, part(pos + away), :], k_sem.at[chips + slot, away])
    arrived(all_ref.at[other], p_send.at[len(order), 0], p_recv.at[len(order), 0])
    keep(all_ref.at[other], out_ref.at[other], k_sem.at[chips + len(order), 0])
    passed = 4 * (1 - core)
    halo_arrived(passed)
    halo_send(window_slot(passed), mw_ref.at[passed], 3 - 2 * core, partner)
    halo_arrived(4 - passed)
    halo_arrived(1)
    halo_arrived(3)
    for copy in kept:
        copy.wait()
    for copy in sends:
        copy.wait_send()


def collect(x_in, marks, w_rows, cols, group, reach):
    tok, dim = x_in.shape
    assert reach == 2
    rows = w_rows.shape[0]
    side = math.isqrt(cols)
    side = side if side * side == cols else 1
    vmem = pl.BlockSpec(memory_space=pltpu.VMEM)
    shards = group // 2
    dma = pltpu.SemaphoreType.DMA
    window = (2 * reach + 1) * tok
    return pl.pallas_call(
        lambda *refs: collect_kernel(cols, group, side, reach, *refs),
        in_specs=[vmem] * 3,
        out_specs=[vmem, vmem, pl.BlockSpec(memory_space=pl.ANY)],
        out_shape=[jax.ShapeDtypeStruct((window, dim), BF16),
                   jax.ShapeDtypeStruct((2 * reach + 1,) + marks.shape, marks.dtype),
                   jax.ShapeDtypeStruct((group, rows, dim), BF16)],
        scratch_shapes=[pltpu.VMEM((group, rows, dim), BF16), dma((shards,)), dma((shards,)), dma((shards, cols)), dma((shards, cols)),
                        dma((shards, cols)), dma((shards, cols)), dma((2 * reach + 1,)), dma((2 * reach + 1,)),
                        dma((2 * reach + 1,)), dma((2 * reach + 1,)), dma((group, cols))],
        compiler_params=pltpu.CompilerParams(collective_id=0, has_side_effects=True, vmem_limit_bytes=VMEM_GRANT),
        cost_estimate=COST,
        name="collect",
    )(x_in, marks, w_rows)


def norm_back(values, d_normed, gain):
    centered = values - jnp.mean(values, axis=-1, keepdims=True)
    rstd = lax.rsqrt(jnp.mean(centered * centered, axis=-1, keepdims=True) + 1e-5)
    unit = centered * rstd
    d_unit = d_normed * gain
    d_val = rstd * (d_unit - jnp.mean(d_unit, axis=-1, keepdims=True)
                    - unit * jnp.mean(d_unit * unit, axis=-1, keepdims=True))
    return d_val, jnp.sum(d_normed * unit, axis=0, keepdims=True)


def reduce_kernel(group, reach, g_ref, du_ref, x_ref, dh_ref, g1_ref, gain2_ref, sum_ref, gx_ref, gains_ref,
                  ring_ref, back_ref, pre_ref, term_ref, r_send, r_recv, h_send, h_recv, t_send, t_recv):
    col, me = lax.axis_index("dp"), lax.axis_index("tp")
    tok = x_ref.shape[0]
    piece = g_ref.shape[1] // (2 * STREAMS)
    up, down = (col, (me + 1) % group), (col, (me + group - 1) % group)
    levels = group.bit_length() - 1

    def flipped(level):
        span = 2 ** level
        return (col, me + span - 2 * span * ((me // span) % 2))

    peers = [(col, (me + by) % group) for by in range(1, reach + 1)]
    peers += [(col, (me + group - by) % group) for by in range(1, reach + 1)]
    peers += [flipped(level) for level in range(levels)]
    barrier = pltpu.get_barrier_semaphore()
    for peer in peers:
        pl.semaphore_signal(barrier, inc=1, device_id=peer, device_id_type=pl.DeviceIdType.MESH)
    pl.semaphore_wait(barrier, len(peers))

    lanes = [(way, part) for part in range(STREAMS) for way in range(2)]

    def rows_of(way, part):
        return pl.ds((way * STREAMS + part) * piece, piece)

    def shard_at(way, hop):
        return (me + 2 * group - 1 - hop) % group if way == 0 else (me + 1 + hop) % group

    for way, part in lanes:
        remote(g_ref.at[shard_at(way, 0), rows_of(way, part), :], ring_ref.at[way, part, 0],
               r_send.at[way, part, 0], r_recv.at[way, part, 0], down if way else up).start()

    chip, core = me // 2, me % 2
    partner = (col, chip * 2 + 1 - core)
    half = tok // 2
    sends = []

    def window_rows(slot):
        return pl.ds(pl.multiple_of(slot * tok, tok), tok)

    def partner_copy(slot, place):
        return remote(du_ref.at[window_rows(slot), :], back_ref.at[place], h_send.at[2 + place], h_recv.at[2 + place], partner)

    def halo_copy(joint, part):
        rows = pl.ds(part * half, half)
        way = core if joint else 1 - core
        src = pre_ref.at[rows, :] if joint else du_ref.at[pl.ds(pl.multiple_of(4 * core * tok + part * half, half), half), :]
        place = 1 - way
        return remote(src, back_ref.at[place, rows, :], h_send.at[2 * place + part], h_recv.at[2 * place + part],
                      (col, (me + group + 2 - 4 * way) % group))

    for slot, place in ((3 - 2 * core, 2), (1 + 2 * core, 3)):
        copy = partner_copy(slot, place)
        copy.start()
        sends.append(copy)
    sends[1].wait_recv()
    pre_ref[...] = (du_ref[window_rows(4 * (1 - core)), :].astype(F32) + back_ref[3].astype(F32)).astype(BF16)

    def ring_step(hop, carry):
        for way, part in lanes:
            slot = ring_ref.at[way, part, hop - 1]
            remote(slot, slot, r_send.at[way, part, hop - 1], r_recv.at[way, part, hop - 1], up).wait_recv()
            mine = g_ref[shard_at(way, hop), rows_of(way, part), :]
            slot[...] = (slot[...].astype(F32) + mine.astype(F32)).astype(BF16)
            remote(slot, ring_ref.at[way, part, hop], r_send.at[way, part, hop], r_recv.at[way, part, hop],
                   down if way else up).start()
        return carry

    for joint in (False, True):
        for part in range(2):
            copy = halo_copy(joint, part)
            copy.start()
            sends.append(copy)
    middle = group // 2
    lax.fori_loop(1, middle, ring_step, 0)

    sends[0].wait_recv()
    for copy in sends[2:]:
        copy.wait_recv()
    total = du_ref[window_rows(reach), :].astype(F32)
    for place in range(3):
        total = total + back_ref[place].astype(F32)
    d_val, g_gain1 = norm_back(x_ref[...].astype(F32), total.astype(BF16).astype(F32), g1_ref[...])
    gx_ref[...] = (dh_ref[...].astype(F32) + d_val.astype(BF16).astype(F32)).astype(BF16)
    term_ref[0, 0] = jnp.zeros(term_ref.shape[2:], F32)
    term_ref[0, 0, 0:1, :] = g_gain1
    term_ref[0, 0, 1:2, :] = gain2_ref[...]
    for level in range(levels):
        ring_step(middle + level, 0)
        copy = remote(term_ref.at[level, 0], term_ref.at[level, 1], t_send.at[level], t_recv.at[level], flipped(level))
        copy.start()
        sends.append(copy)
        copy.wait_recv()
        both = term_ref[level, 0] + term_ref[level, 1]
        if level + 1 < levels:
            term_ref[level + 1, 0] = both
        else:
            gains_ref[...] = both[0:2]
    lax.fori_loop(middle + levels, group - 1, ring_step, 0)

    for way, part in lanes:
        slot = ring_ref.at[way, part, group - 2]
        remote(slot, slot, r_send.at[way, part, group - 2], r_recv.at[way, part, group - 2], up).wait_recv()
        sum_ref[rows_of(way, part), :] = slot[...].astype(F32) + g_ref[me, rows_of(way, part), :].astype(F32)
    for copy in sends:
        copy.wait_send()

    def drain(hop, carry):
        for way, part in lanes:
            slot = ring_ref.at[way, part, hop]
            remote(slot, slot, r_send.at[way, part, hop], r_recv.at[way, part, hop], up).wait_send()
        return carry

    lax.fori_loop(0, group - 1, drain, 0)


def reduce_rows(g_att, du_win, x_in, d_hidden, gain1, g_gain2, reach):
    group, rows, dim = g_att.shape
    assert reach == 2
    tok = x_in.shape[0]
    levels = group.bit_length() - 1
    piece = rows // (2 * STREAMS)
    vmem = pl.BlockSpec(memory_space=pltpu.VMEM)
    dma = pltpu.SemaphoreType.DMA
    return pl.pallas_call(
        lambda *refs: reduce_kernel(group, reach, *refs),
        in_specs=[vmem] * 6,
        out_specs=[vmem] * 3,
        out_shape=[jax.ShapeDtypeStruct((rows, dim), F32), jax.ShapeDtypeStruct((tok, dim), BF16),
                   jax.ShapeDtypeStruct((2, dim), F32)],
        scratch_shapes=[pltpu.VMEM((2, STREAMS, group - 1, piece, dim), BF16),
                        pltpu.VMEM((4, tok, dim), BF16), pltpu.VMEM((tok, dim), BF16),
                        pltpu.VMEM((levels, 2, 8, dim), F32),
                        dma((2, STREAMS, group - 1)), dma((2, STREAMS, group - 1)),
                        dma((6,)), dma((6,)), dma((levels,)), dma((levels,))],
        compiler_params=pltpu.CompilerParams(collective_id=1, has_side_effects=True, vmem_limit_bytes=VMEM_GRANT),
        cost_estimate=COST,
        name="reduce",
    )(g_att, du_win, x_in, d_hidden, gain1, g_gain2)


def whole(shape):
    return pl.BlockSpec(shape, lambda i: (0,) * len(shape))


def stepped(*shape):
    return pl.BlockSpec(shape, lambda i: (i,) + (0,) * (len(shape) - 1))


def attn_forward(x_win, gain1, gain2, w_att, cos_t, sin_t, seg_col, seg_row, tok, heads):
    win, dim = x_win.shape
    halo = (win - tok) // 2
    per = math.gcd(heads, HEADS_STEP)
    steps = heads // per
    feat = per * HEAD_DIM
    return pl.pallas_call(
        lambda *refs: attn_fwd_kernel(halo, tok, *refs),
        grid=(steps,),
        in_specs=[whole((win, dim)), whole((1, dim)), whole((1, dim)),
                  stepped(per, 4, HEAD_DIM, dim),
                  whole((HALF, win)), whole((HALF, win)), whole((win, 1)), whole((1, tok))],
        out_specs=[whole((win, dim)),
                   stepped(feat, tok),
                   stepped(feat, win),
                   stepped(feat, win),
                   stepped(feat, tok),
                   stepped(1, per, tok),
                   whole((tok, dim)), whole((tok, dim))],
        out_shape=[jax.ShapeDtypeStruct((win, dim), BF16),
                   jax.ShapeDtypeStruct((heads * HEAD_DIM, tok), BF16),
                   jax.ShapeDtypeStruct((heads * HEAD_DIM, win), BF16),
                   jax.ShapeDtypeStruct((heads * HEAD_DIM, win), BF16),
                   jax.ShapeDtypeStruct((heads * HEAD_DIM, tok), BF16),
                   jax.ShapeDtypeStruct((steps, per, tok), F32),
                   jax.ShapeDtypeStruct((tok, dim), BF16),
                   jax.ShapeDtypeStruct((tok, dim), BF16)],
        scratch_shapes=[pltpu.VMEM((win, tok), F32), pltpu.VMEM((tok, dim), F32)],
        compiler_params=pltpu.CompilerParams(dimension_semantics=("arbitrary",), vmem_limit_bytes=VMEM_GRANT),
        cost_estimate=COST,
        name="attn_fwd",
    )(x_win, gain1, gain2, w_att, cos_t, sin_t, seg_col, seg_row)


def mlp(normed2, hidden, grad_out, gain2, w_first, w_rest, rows):
    tok, dim = normed2.shape
    shards = w_rest.shape[0]
    parts = 3
    per = math.gcd(shards, MLP_SHARDS)
    block = stepped(per, parts, rows, dim)
    return pl.pallas_call(
        mlp_kernel,
        grid=(shards // per,),
        in_specs=[whole((tok, dim)), whole((tok, dim)), whole((tok, dim)), whole((1, dim)),
                  pl.BlockSpec((per, EXTRA // HEAD_DIM, HEAD_DIM, dim), lambda i: (i, w_first.shape[1] * HEAD_DIM // EXTRA - 1, 0, 0)),
                  stepped(per, w_rest.shape[1], dim)],
        out_specs=[block, whole((tok, dim)), whole((tok, dim)), whole((1, dim))],
        out_shape=[jax.ShapeDtypeStruct((shards, parts, rows, dim), BF16),
                   jax.ShapeDtypeStruct((tok, dim), BF16),
                   jax.ShapeDtypeStruct((tok, dim), BF16),
                   jax.ShapeDtypeStruct((1, dim), F32)],
        scratch_shapes=[pltpu.VMEM((tok, dim), F32), pltpu.VMEM((tok, dim), F32)],
        compiler_params=pltpu.CompilerParams(dimension_semantics=("arbitrary",), vmem_limit_bytes=VMEM_GRANT),
        cost_estimate=COST,
        name="mlp",
    )(normed2, hidden, grad_out, gain2, w_first, w_rest)


def attn_backward(u_win, d_hid, w_att, cos_t, sin_t, seg_col, seg_row, q_t, k_t, v_t, o_t, lse, heads):
    win, dim = u_win.shape
    tok = d_hid.shape[0]
    halo = (win - tok) // 2
    per = math.gcd(heads, HEADS_STEP)
    steps = heads // per
    feat = per * HEAD_DIM
    return pl.pallas_call(
        lambda *refs: attn_bwd_kernel(halo, tok, *refs),
        grid=(steps,),
        in_specs=[whole((win, dim)), whole((tok, dim)),
                  stepped(per, 4, HEAD_DIM, dim),
                  whole((HALF, win)), whole((HALF, win)), whole((win, 1)), whole((1, tok)),
                  stepped(feat, tok),
                  stepped(feat, win),
                  stepped(feat, win),
                  stepped(feat, tok),
                  stepped(1, per, tok)],
        out_specs=[stepped(per, 4, HEAD_DIM, dim), whole((win, dim))],
        out_shape=[jax.ShapeDtypeStruct((heads, 4, HEAD_DIM, dim), BF16),
                   jax.ShapeDtypeStruct((win, dim), BF16)],
        scratch_shapes=[pltpu.VMEM((win, tok), F32), pltpu.VMEM((win, dim), F32)],
        compiler_params=pltpu.CompilerParams(dimension_semantics=("arbitrary",), vmem_limit_bytes=VMEM_GRANT),
        cost_estimate=COST,
        name="attn_bwd",
    )(u_win, d_hid, w_att, cos_t, sin_t, seg_col, seg_row, q_t, k_t, v_t, o_t, lse)


def solution(mesh):
    tok_spec = P(('dp', 'tp'), None)
    seq_spec = P(('dp', 'tp'))
    in_specs = (tok_spec, seq_spec, seq_spec, P(None), P(None, None, 'tp'), P('tp', None),
                P(None), P(None, None, 'tp'), P('tp', None), tok_spec)
    out_specs = (tok_spec, tok_spec, P('dp'), P('dp', None, 'tp'), P(('dp', 'tp'), None),
                 P('dp'), P('dp', None, 'tp'), P(('dp', 'tp'), None))
    group = mesh.shape['tp']
    cols = mesh.shape['dp']

    def gather_rows(shard_rows):
        return lax.all_gather(shard_rows, 'tp', axis=0, tiled=True)

    def scatter_rows(part_sum):
        return lax.psum_scatter(part_sum, 'tp', scatter_dimension=0, tiled=True)

    def device_step(x_in, doc_ids, doc_pos, gamma1, w_qkv, w_out, gamma2, w_in, w_down, grad_out):
        tok, dim = x_in.shape
        heads_loc = w_qkv.shape[2] // HEAD_DIM
        ff_loc = w_in.shape[2]
        ff_pad = -(-ff_loc // FF_ALIGN) * FF_ALIGN
        reach = -(-MAX_DOC // tok)
        qkv_rows = jnp.transpose(w_qkv.reshape(dim, 3, heads_loc, HEAD_DIM), (2, 1, 3, 0))
        out_rows = w_out.reshape(heads_loc, 1, HEAD_DIM, dim)
        att_rows = jnp.concatenate([qkv_rows, out_rows], axis=1)
        mlp_rows = jnp.concatenate([jnp.transpose(w_in, (1, 2, 0)), w_down[None]], axis=0)
        mlp_rows = jnp.pad(mlp_rows, ((0, 0), (0, ff_pad - ff_loc), (0, 0))).reshape(3 * ff_pad, dim)
        first_rows = jnp.concatenate([att_rows.reshape(-1, dim), mlp_rows[:EXTRA]], axis=0)
        x_win, marks, w_first = collect(x_in, jnp.stack([doc_ids, doc_pos]), first_rows, cols, group, reach)
        w_rest = gather_rows(mlp_rows[EXTRA:]).reshape(group, 3 * ff_pad - EXTRA, dim)
        w_first = w_first.reshape(group, -1, HEAD_DIM, dim)
        seg_row, seg_col = doc_ids[None, :], marks[:, 0].reshape(-1, 1)
        inv_freq = 160000.0 ** (-jnp.arange(HALF, dtype=F32) / HALF)
        angle = marks[:, 1].reshape(1, -1).astype(F32) * inv_freq[:, None]
        cos_t, sin_t = jnp.cos(angle), jnp.sin(angle)


        gain1 = gamma1.astype(F32)[None, :]
        gain2 = gamma2.astype(F32)[None, :]
        u_win, q_t, k_t, v_t, o_t, lse, hidden, normed2 = attn_forward(
            x_win, gain1, gain2, w_first, cos_t, sin_t, seg_col, seg_row, tok, group * heads_loc)
        g_mlp, layer_out, d_hidden, g_gain2 = mlp(normed2, hidden, grad_out, gain2, w_first, w_rest, ff_pad)
        g_mlp = scatter_rows(g_mlp.reshape(group * 3 * ff_pad, dim))
        g_att, du_win = attn_backward(u_win, d_hidden, w_first, cos_t, sin_t, seg_col, seg_row,
                                      q_t, k_t, v_t, o_t, lse, group * heads_loc)
        g_att, grad_x, gains = reduce_rows(g_att.reshape(group, heads_loc * 4 * HEAD_DIM, dim), du_win, x_in,
                                           d_hidden, gain1, g_gain2, reach)

        g_att = g_att.reshape(heads_loc, 4, HEAD_DIM, dim)
        g_qkv = jnp.transpose(g_att[:, :3], (3, 1, 0, 2)).reshape(dim, 3, heads_loc * HEAD_DIM)
        g_out = g_att[:, 3].reshape(heads_loc * HEAD_DIM, dim)
        g_mlp = g_mlp.reshape(3, ff_pad, dim)[:, :ff_loc].astype(F32)
        g_in = jnp.transpose(g_mlp[:2], (2, 0, 1))
        return (layer_out, grad_x, gains[0], g_qkv, g_out, gains[1], g_in, g_mlp[2])

    return jax.shard_map(device_step, mesh=mesh, in_specs=in_specs, out_specs=out_specs, check_vma=False)
```

```python
import math
import jax
import jax.numpy as jnp
from jax import lax
from jax.experimental import pallas as pl
from jax.experimental.pallas import tpu as pltpu
from jax.sharding import PartitionSpec as P

MAX_DOC = 512
HEAD_DIM = 64
HALF = HEAD_DIM // 2
VMEM_GRANT = 60 * 2 ** 20
FF_ALIGN = 8
MLP_SHARDS = 4
HEADS_STEP = 4
EXTRA = 256
STREAMS = 2
LOG2E = 1.4426950408889634
S_SCALE = 0.125 * LOG2E
NEG = -1e30
SQRT_HALF = 0.7071067811865476
INV_SQRT_2PI = 0.3989422804014327
F32 = jnp.float32
BF16 = jnp.bfloat16
COST = pl.CostEstimate(flops=30_000_000_000, bytes_accessed=30_000_000, transcendentals=5_000_000)


def layer_norm(values, gain):
    vals32 = values.astype(F32)
    mean_val = jnp.mean(vals32, axis=-1, keepdims=True)
    centered = vals32 - mean_val
    var_val = jnp.mean(centered * centered, axis=-1, keepdims=True)
    return (centered * lax.rsqrt(var_val + 1e-5) * gain).astype(BF16)


def dot_nn(a, b):
    return lax.dot_general(a, b, (((1,), (0,)), ((), ())), preferred_element_type=F32)


def dot_nt(a, b):
    return lax.dot_general(a, b, (((1,), (1,)), ((), ())), preferred_element_type=F32)


def dot_tn(a, b):
    return lax.dot_general(a, b, (((0,), (0,)), ((), ())), preferred_element_type=F32)


def flip(vals):
    return vals.astype(F32).T.astype(BF16)


def rope_fwd(vals_t, cos_t, sin_t):
    rows = []
    for head in range(vals_t.shape[0] // HEAD_DIM):
        lo = vals_t[head * HEAD_DIM: head * HEAD_DIM + HALF]
        hi = vals_t[head * HEAD_DIM + HALF: (head + 1) * HEAD_DIM]
        rows += [lo * cos_t - hi * sin_t, hi * cos_t + lo * sin_t]
    return jnp.concatenate(rows, axis=0)


def rope_back(lo, hi, cos_t, sin_t):
    return [lo * cos_t + hi * sin_t, hi * cos_t - lo * sin_t]


def attn_fwd_kernel(halo, tok, x_ref, g1_ref, g2_ref, w_ref, cos_ref, sin_ref, segc_ref, segr_ref,
                    u_ref, qt_ref, kt_ref, vt_ref, ot_ref, lse_ref, hid_ref, n2_ref, bias_ref, att_ref):
    own = pl.ds(halo, tok)
    step = pl.program_id(0)

    @pl.when(step == 0)
    def _():
        u_ref[...] = layer_norm(x_ref[...], g1_ref[...])
        bias_ref[...] = jnp.where(segc_ref[...] == segr_ref[...], 0.0, NEG).astype(F32)
        att_ref[...] = jnp.zeros_like(att_ref)

    heads, wide = w_ref.shape[0], w_ref.shape[3]
    w_q, w_k, w_v, w_o = [w_ref[:, part].reshape(heads * HEAD_DIM, wide) for part in range(4)]
    u_win = u_ref[...]
    u_own = u_ref[own, :]
    q_raw = dot_nt(w_q, u_own).astype(BF16).astype(F32)
    k_raw = dot_nt(w_k, u_win).astype(BF16).astype(F32)
    v_t = dot_nt(w_v, u_win).astype(BF16)
    q_t = rope_fwd(q_raw, cos_ref[:, halo:halo + tok], sin_ref[:, halo:halo + tok]).astype(BF16)
    k_t = rope_fwd(k_raw, cos_ref[...], sin_ref[...]).astype(BF16)
    qt_ref[...] = q_t
    kt_ref[...] = k_t
    vt_ref[...] = v_t
    for head in range(heads):
        rows = slice(head * HEAD_DIM, (head + 1) * HEAD_DIM)
        score = dot_nn(flip(k_t[rows]), q_t[rows]) * S_SCALE + bias_ref[...]
        top = jnp.max(score, axis=0, keepdims=True)
        expd = jnp.exp2(score - top)
        total = jnp.sum(expd, axis=0, keepdims=True)
        prob = (expd * (1.0 / total)).astype(BF16)
        ot_ref[rows, :] = dot_nn(v_t[rows], prob).astype(BF16)
        lse_ref[0, head:head + 1, :] = top + jnp.log2(total)
    att_ref[...] += dot_nn(flip(ot_ref[...]), w_o)

    @pl.when(step == pl.num_programs(0) - 1)
    def _():
        hidden = (x_ref[own, :].astype(F32) + att_ref[...].astype(BF16).astype(F32)).astype(BF16)
        hid_ref[...] = hidden
        n2_ref[...] = layer_norm(hidden, g2_ref[...])


def mlp_kernel(n2_ref, hid_ref, go_ref, g2_ref, we_ref, wr_ref, g_ref, out_ref, dh_ref, gain_ref, mlp_ref, dn_ref):
    step = pl.program_id(0)

    @pl.when(step == 0)
    def _():
        mlp_ref[...] = jnp.zeros_like(mlp_ref)
        dn_ref[...] = jnp.zeros_like(dn_ref)

    n2 = n2_ref[...]
    g_out = go_ref[...]
    per, _, rows, wide = g_ref.shape
    lead = we_ref.shape[1] * we_ref.shape[2]
    first, rest = we_ref[...].reshape(per, lead, wide), wr_ref[...]
    w_a = first[:, :rows].reshape(per * rows, wide)
    w_b = jnp.concatenate([first[:, rows:], rest[:, :2 * rows - lead]], axis=1).reshape(per * rows, wide)
    w_d = rest[:, 2 * rows - lead:].reshape(per * rows, wide)
    gate = dot_nt(w_a, n2).astype(BF16).astype(F32)
    lin = dot_nt(w_b, n2).astype(BF16).astype(F32)
    cdf = 0.5 * (1.0 + lax.erf(gate * SQRT_HALF))
    act = gate * cdf
    gated = (act * lin).astype(BF16)
    d_gated = dot_nt(w_d, g_out).astype(BF16).astype(F32)
    slope = cdf + gate * (jnp.exp2(gate * gate * (-0.5 * LOG2E)) * INV_SQRT_2PI)
    d_gate = (d_gated * lin * slope).astype(BF16)
    d_lin = (d_gated * act).astype(BF16)
    mlp_ref[...] += dot_nn(flip(gated), w_d)
    dn_ref[...] += dot_nn(flip(d_gate), w_a) + dot_nn(flip(d_lin), w_b)
    g_ref[:, 0] = dot_nn(d_gate, n2).astype(BF16).reshape(per, rows, wide)
    g_ref[:, 1] = dot_nn(d_lin, n2).astype(BF16).reshape(per, rows, wide)
    g_ref[:, 2] = dot_nn(gated, g_out).astype(BF16).reshape(per, rows, wide)

    @pl.when(step == pl.num_programs(0) - 1)
    def _():
        hidden = hid_ref[...].astype(F32)
        out_ref[...] = (hidden + mlp_ref[...].astype(BF16).astype(F32)).astype(BF16)
        d_n2 = dn_ref[...].astype(BF16).astype(F32)
        d_hid, gain_ref[...] = norm_back(hidden, d_n2, g2_ref[...])
        dh_ref[...] = (g_out.astype(F32) + d_hid.astype(BF16).astype(F32)).astype(BF16)


def attn_bwd_kernel(halo, tok, u_ref, dh_ref, w_ref, cos_ref, sin_ref, segc_ref, segr_ref,
                    qt_ref, kt_ref, vt_ref, ot_ref, lse_ref, g_ref, du_ref, bias_ref, acc_ref):
    own = pl.ds(halo, tok)
    step = pl.program_id(0)

    @pl.when(step == 0)
    def _():
        bias_ref[...] = jnp.where(segc_ref[...] == segr_ref[...], 0.0, NEG).astype(F32)

    heads, wide = w_ref.shape[0], w_ref.shape[3]
    d_hid = dh_ref[...]
    do_t = dot_nt(w_ref[:, 3].reshape(heads * HEAD_DIM, wide), d_hid).astype(BF16)
    o_t = ot_ref[...]
    g_ref[:, 3] = dot_nn(o_t, d_hid).astype(BF16).reshape(heads, HEAD_DIM, wide)
    cos_w, sin_w = cos_ref[...], sin_ref[...]
    cos_o, sin_o = cos_ref[:, halo:halo + tok], sin_ref[:, halo:halo + tok]
    dq_rows, dk_rows, dv_rows = [], [], []
    for head in range(heads):
        rows = slice(head * HEAD_DIM, (head + 1) * HEAD_DIM)
        q_t, k_t, v_t, d_o = qt_ref[rows, :], kt_ref[rows, :], vt_ref[rows, :], do_t[rows]
        score = dot_nn(flip(k_t), q_t) * S_SCALE + bias_ref[...]
        prob = jnp.exp2(score - lse_ref[0, head:head + 1, :])
        delta = jnp.sum(d_o.astype(F32) * o_t[rows].astype(F32), axis=0, keepdims=True)
        d_prob = dot_nn(flip(v_t), d_o).astype(BF16).astype(F32)
        d_score = (prob * (d_prob - delta)).astype(BF16)
        dv_rows.append(dot_nt(d_o, prob.astype(BF16)).astype(BF16))
        d_q = (dot_nn(k_t, d_score) * 0.125).astype(BF16).astype(F32)
        d_k = (dot_nt(q_t, d_score) * 0.125).astype(BF16).astype(F32)
        dq_rows += rope_back(d_q[:HALF], d_q[HALF:], cos_o, sin_o)
        dk_rows += rope_back(d_k[:HALF], d_k[HALF:], cos_w, sin_w)
    dq_t = jnp.concatenate(dq_rows, axis=0).astype(BF16)
    dk_t = jnp.concatenate(dk_rows, axis=0).astype(BF16)
    dv_t = jnp.concatenate(dv_rows, axis=0)
    u_win = u_ref[...]
    g_ref[:, 0] = dot_nn(dq_t, u_ref[own, :]).astype(BF16).reshape(heads, HEAD_DIM, wide)
    g_ref[:, 1] = dot_nn(dk_t, u_win).astype(BF16).reshape(heads, HEAD_DIM, wide)
    g_ref[:, 2] = dot_nn(dv_t, u_win).astype(BF16).reshape(heads, HEAD_DIM, wide)
    w_q = w_ref[:, 0].reshape(heads * HEAD_DIM, wide)
    w_kv = jnp.concatenate([w_ref[:, 1].reshape(heads * HEAD_DIM, wide), w_ref[:, 2].reshape(heads * HEAD_DIM, wide)], axis=0)
    d_kv = jnp.concatenate([flip(dk_t), flip(dv_t)], axis=1)
    term = dot_nn(d_kv, w_kv)

    @pl.when(step == 0)
    def _():
        acc_ref[...] = term

    @pl.when(step > 0)
    def _():
        acc_ref[...] += term

    acc_ref[own, :] += dot_nn(flip(dq_t), w_q)

    @pl.when(step == pl.num_programs(0) - 1)
    def _():
        du_ref[...] = acc_ref[...].astype(BF16)


def remote(src, dst, send_sem, recv_sem, where):
    return pltpu.make_async_remote_copy(src_ref=src, dst_ref=dst, send_sem=send_sem, recv_sem=recv_sem,
                                        device_id=where, device_id_type=pl.DeviceIdType.MESH)


def collect_kernel(cols, group, side, reach, x_ref, m_ref, w_ref, xw_ref, mw_ref, out_ref, all_ref,
                   z_send, z_recv, c_send, c_recv, p_send, p_recv, h_send, h_recv, m_send, m_recv, k_sem):
    col, me = lax.axis_index("dp"), lax.axis_index("tp")
    chips = group // 2
    chip, core = me // 2, me % 2
    tok = x_ref.shape[0]
    part_rows = w_ref.shape[0] // cols

    def column_at(pos):
        line, off = pos // side, pos % side
        return line * side + off + (line % 2) * (side - 1 - 2 * off)

    line, off = col // side, col % side
    pos = line * side + off + (line % 2) * (side - 1 - 2 * off)
    right_col, left_col = column_at((pos + 1) % cols), column_at((pos + cols - 1) % cols)
    partner = (col, chip * 2 + 1 - core)
    ahead, behind = (col, (me + 2) % group), (col, (me + group - 2) % group)

    peers = [(col, (me + by) % group) for by in range(1, reach + 1)]
    peers += [(col, (me + group - by) % group) for by in range(1, reach + 1)]
    if cols > 1:
        peers += [(right_col, me)]
    if cols > 2:
        peers += [(left_col, me)]
    barrier = pltpu.get_barrier_semaphore()
    for peer in peers:
        pl.semaphore_signal(barrier, inc=1, device_id=peer, device_id_type=pl.DeviceIdType.MESH)
    pl.semaphore_wait(barrier, len(peers))

    def part(pos_of):
        return pl.ds(pl.multiple_of((pos_of % cols) * part_rows, part_rows), part_rows)

    sends = []

    def send(src, dst, s_sem, r_sem, where):
        copy = remote(src, dst, s_sem, r_sem, where)
        copy.start()
        sends.append(copy)

    def arrived(dst, s_sem, r_sem):
        remote(dst, dst, s_sem, r_sem, partner).wait_recv()

    kept = []

    def keep(src, dst, sem):
        copy = pltpu.make_async_copy(src, dst, sem)
        copy.start()
        kept.append(copy)

    fwd_hops, back_hops = chips // 2, (chips - 1) // 2
    order = []
    for hop in range(1, fwd_hops + 1):
        order.append((1, hop))
        if hop <= back_hops:
            order.append((-1, hop))
    number = {key: slot for slot, key in enumerate(order)}

    own_part = w_ref.at[part(pos), :]
    send(own_part, all_ref.at[me, part(pos), :], z_send.at[number[1, 1]], z_recv.at[number[1, 1]], ahead)
    send(own_part, all_ref.at[me, part(pos), :], z_send.at[number[-1, 1]], z_recv.at[number[-1, 1]], behind)
    send(w_ref, all_ref.at[me], p_send.at[len(order), 0], p_recv.at[len(order), 0], partner)
    keep(w_ref, out_ref.at[me], k_sem.at[len(order), 0])
    xw_ref[pl.ds(reach * tok, tok), :] = x_ref[...]
    mw_ref[reach] = m_ref[...]

    def shard_of(slot):
        way, hop = order[slot]
        return ((chip + chips - way * hop) % chips) * 2 + core

    def hops_of(slot):
        right = (cols - 1 + slot % 2) // 2
        return right, cols - 1 - right

    for slot, (way, hop) in enumerate(order):
        place = all_ref.at[shard_of(slot), part(pos), :]
        arrived(place, z_send.at[slot], z_recv.at[slot])
        keep(place, out_ref.at[shard_of(slot), part(pos), :], k_sem.at[slot, 0])
        nxt = number.get((way, hop + 1))
        if nxt is not None:
            send(place, place, z_send.at[nxt], z_recv.at[nxt], ahead if way > 0 else behind)
        right, left = hops_of(slot)
        if right > 0:
            send(place, place, c_send.at[slot, cols - 1], c_recv.at[slot, cols - 1], (right_col, me))
        if left > 0:
            send(place, place, c_send.at[slot, 1], c_recv.at[slot, 1], (left_col, me))
        send(place, place, p_send.at[slot, 0], p_recv.at[slot, 0], partner)
    def window_slot(slot):
        return xw_ref.at[pl.ds(pl.multiple_of(slot * tok, tok), tok), :]

    def halo_send(src, marks, slot, where):
        send(src, window_slot(slot), h_send.at[slot], h_recv.at[slot], where)
        send(marks, mw_ref.at[slot], m_send.at[slot], m_recv.at[slot], where)

    def halo_arrived(slot):
        arrived(window_slot(slot), h_send.at[slot], h_recv.at[slot])
        arrived(mw_ref.at[slot], m_send.at[slot], m_recv.at[slot])

    halo_send(x_ref, m_ref, 0, ahead)
    halo_send(x_ref, m_ref, 4, behind)
    halo_send(x_ref, m_ref, 1 + 2 * core, partner)
    for hop in range(1, cols // 2 + 1):
        for slot in range(len(order)):
            right, left = hops_of(slot)
            if hop <= right:
                place = all_ref.at[shard_of(slot), part(pos + cols - hop), :]
                arrived(place, c_send.at[slot, cols - hop], c_recv.at[slot, cols - hop])
                keep(place, out_ref.at[shard_of(slot), part(pos + cols - hop), :], k_sem.at[slot, cols - hop])
                if hop < right:
                    send(place, place, c_send.at[slot, cols - hop - 1], c_recv.at[slot, cols - hop - 1], (right_col, me))
                send(place, place, p_send.at[slot, cols - hop], p_recv.at[slot, cols - hop], partner)
            if hop <= left:
                place = all_ref.at[shard_of(slot), part(pos + hop), :]
                arrived(place, c_send.at[slot, hop], c_recv.at[slot, hop])
                keep(place, out_ref.at[shard_of(slot), part(pos + hop), :], k_sem.at[slot, hop])
                if hop < left:
                    send(place, place, c_send.at[slot, hop + 1], c_recv.at[slot, hop + 1], (left_col, me))
                send(place, place, p_send.at[slot, hop], p_recv.at[slot, hop], partner)
    other = chip * 2 + 1 - core
    for slot in range(len(order)):
        shard = shard_of(slot) + 1 - 2 * core
        for away in range(cols):
            place = all_ref.at[shard, part(pos + away), :]
            arrived(place, p_send.at[slot, away], p_recv.at[slot, away])
            keep(place, out_ref.at[shard, part(pos + away), :], k_sem.at[chips + slot, away])
    arrived(all_ref.at[other], p_send.at[len(order), 0], p_recv.at[len(order), 0])
    keep(all_ref.at[other], out_ref.at[other], k_sem.at[chips + len(order), 0])
    passed = 4 * (1 - core)
    halo_arrived(passed)
    halo_send(window_slot(passed), mw_ref.at[passed], 3 - 2 * core, partner)
    halo_arrived(4 - passed)
    halo_arrived(1)
    halo_arrived(3)
    for copy in kept:
        copy.wait()
    for copy in sends:
        copy.wait_send()


def collect(x_in, marks, w_rows, cols, group, reach):
    tok, dim = x_in.shape
    assert reach == 2
    rows = w_rows.shape[0]
    side = math.isqrt(cols)
    side = side if side * side == cols else 1
    vmem = pl.BlockSpec(memory_space=pltpu.VMEM)
    shards = group // 2
    dma = pltpu.SemaphoreType.DMA
    window = (2 * reach + 1) * tok
    return pl.pallas_call(
        lambda *refs: collect_kernel(cols, group, side, reach, *refs),
        in_specs=[vmem] * 3,
        out_specs=[vmem, vmem, pl.BlockSpec(memory_space=pl.ANY)],
        out_shape=[jax.ShapeDtypeStruct((window, dim), BF16),
                   jax.ShapeDtypeStruct((2 * reach + 1,) + marks.shape, marks.dtype),
                   jax.ShapeDtypeStruct((group, rows, dim), BF16)],
        scratch_shapes=[pltpu.VMEM((group, rows, dim), BF16), dma((shards,)), dma((shards,)), dma((shards, cols)), dma((shards, cols)),
                        dma((shards, cols)), dma((shards, cols)), dma((2 * reach + 1,)), dma((2 * reach + 1,)),
                        dma((2 * reach + 1,)), dma((2 * reach + 1,)), dma((group, cols))],
        compiler_params=pltpu.CompilerParams(collective_id=0, has_side_effects=True, vmem_limit_bytes=VMEM_GRANT),
        cost_estimate=COST,
        name="collect",
    )(x_in, marks, w_rows)


def norm_back(values, d_normed, gain):
    centered = values - jnp.mean(values, axis=-1, keepdims=True)
    rstd = lax.rsqrt(jnp.mean(centered * centered, axis=-1, keepdims=True) + 1e-5)
    unit = centered * rstd
    d_unit = d_normed * gain
    d_val = rstd * (d_unit - jnp.mean(d_unit, axis=-1, keepdims=True)
                    - unit * jnp.mean(d_unit * unit, axis=-1, keepdims=True))
    return d_val, jnp.sum(d_normed * unit, axis=0, keepdims=True)


def reduce_kernel(group, reach, g_ref, du_ref, x_ref, dh_ref, g1_ref, gain2_ref, sum_ref, gx_ref, gains_ref,
                  ring_ref, back_ref, pre_ref, term_ref, r_send, r_recv, h_send, h_recv, t_send, t_recv):
    col, me = lax.axis_index("dp"), lax.axis_index("tp")
    tok = x_ref.shape[0]
    piece = g_ref.shape[1] // (2 * STREAMS)
    up, down = (col, (me + 1) % group), (col, (me + group - 1) % group)
    levels = group.bit_length() - 1

    def flipped(level):
        span = 2 ** level
        return (col, me + span - 2 * span * ((me // span) % 2))

    peers = [(col, (me + by) % group) for by in range(1, reach + 1)]
    peers += [(col, (me + group - by) % group) for by in range(1, reach + 1)]
    peers += [flipped(level) for level in range(levels)]
    barrier = pltpu.get_barrier_semaphore()
    for peer in peers:
        pl.semaphore_signal(barrier, inc=1, device_id=peer, device_id_type=pl.DeviceIdType.MESH)
    pl.semaphore_wait(barrier, len(peers))

    lanes = [(way, part) for part in range(STREAMS) for way in range(2)]

    def rows_of(way, part):
        return pl.ds((way * STREAMS + part) * piece, piece)

    def shard_at(way, hop):
        return (me + 2 * group - 1 - hop) % group if way == 0 else (me + 1 + hop) % group

    for way, part in lanes:
        remote(g_ref.at[shard_at(way, 0), rows_of(way, part), :], ring_ref.at[way, part, 0],
               r_send.at[way, part, 0], r_recv.at[way, part, 0], down if way else up).start()

    chip, core = me // 2, me % 2
    partner = (col, chip * 2 + 1 - core)
    half = tok // 2
    sends = []

    def window_rows(slot):
        return pl.ds(pl.multiple_of(slot * tok, tok), tok)

    def partner_copy(slot, place):
        return remote(du_ref.at[window_rows(slot), :], back_ref.at[place], h_send.at[2 + place], h_recv.at[2 + place], partner)

    def halo_copy(joint, part):
        rows = pl.ds(part * half, half)
        way = core if joint else 1 - core
        src = pre_ref.at[rows, :] if joint else du_ref.at[pl.ds(pl.multiple_of(4 * core * tok + part * half, half), half), :]
        place = 1 - way
        return remote(src, back_ref.at[place, rows, :], h_send.at[2 * place + part], h_recv.at[2 * place + part],
                      (col, (me + group + 2 - 4 * way) % group))

    for slot, place in ((3 - 2 * core, 2), (1 + 2 * core, 3)):
        copy = partner_copy(slot, place)
        copy.start()
        sends.append(copy)
    sends[1].wait_recv()
    pre_ref[...] = (du_ref[window_rows(4 * (1 - core)), :].astype(F32) + back_ref[3].astype(F32)).astype(BF16)

    def ring_step(hop, carry):
        for way, part in lanes:
            slot = ring_ref.at[way, part, hop - 1]
            remote(slot, slot, r_send.at[way, part, hop - 1], r_recv.at[way, part, hop - 1], up).wait_recv()
            mine = g_ref[shard_at(way, hop), rows_of(way, part), :]
            slot[...] = (slot[...].astype(F32) + mine.astype(F32)).astype(BF16)
            remote(slot, ring_ref.at[way, part, hop], r_send.at[way, part, hop], r_recv.at[way, part, hop],
                   down if way else up).start()
        return carry

    for joint in (False, True):
        for part in range(2):
            copy = halo_copy(joint, part)
            copy.start()
            sends.append(copy)
    middle = group // 2
    lax.fori_loop(1, middle, ring_step, 0)

    sends[0].wait_recv()
    for copy in sends[2:]:
        copy.wait_recv()
    total = du_ref[window_rows(reach), :].astype(F32)
    for place in range(3):
        total = total + back_ref[place].astype(F32)
    d_val, g_gain1 = norm_back(x_ref[...].astype(F32), total.astype(BF16).astype(F32), g1_ref[...])
    gx_ref[...] = (dh_ref[...].astype(F32) + d_val.astype(BF16).astype(F32)).astype(BF16)
    term_ref[0, 0] = jnp.zeros(term_ref.shape[2:], F32)
    term_ref[0, 0, 0:1, :] = g_gain1
    term_ref[0, 0, 1:2, :] = gain2_ref[...]
    for level in range(levels):
        ring_step(middle + level, 0)
        copy = remote(term_ref.at[level, 0], term_ref.at[level, 1], t_send.at[level], t_recv.at[level], flipped(level))
        copy.start()
        sends.append(copy)
        copy.wait_recv()
        both = term_ref[level, 0] + term_ref[level, 1]
        if level + 1 < levels:
            term_ref[level + 1, 0] = both
        else:
            gains_ref[...] = both[0:2]
    lax.fori_loop(middle + levels, group - 1, ring_step, 0)

    for way, part in lanes:
        slot = ring_ref.at[way, part, group - 2]
        remote(slot, slot, r_send.at[way, part, group - 2], r_recv.at[way, part, group - 2], up).wait_recv()
        sum_ref[rows_of(way, part), :] = slot[...].astype(F32) + g_ref[me, rows_of(way, part), :].astype(F32)
    for copy in sends:
        copy.wait_send()

    def drain(hop, carry):
        for way, part in lanes:
            slot = ring_ref.at[way, part, hop]
            remote(slot, slot, r_send.at[way, part, hop], r_recv.at[way, part, hop], up).wait_send()
        return carry

    lax.fori_loop(0, group - 1, drain, 0)


def reduce_rows(g_att, du_win, x_in, d_hidden, gain1, g_gain2, reach):
    group, rows, dim = g_att.shape
    assert reach == 2
    tok = x_in.shape[0]
    levels = group.bit_length() - 1
    piece = rows // (2 * STREAMS)
    vmem = pl.BlockSpec(memory_space=pltpu.VMEM)
    dma = pltpu.SemaphoreType.DMA
    return pl.pallas_call(
        lambda *refs: reduce_kernel(group, reach, *refs),
        in_specs=[vmem] * 6,
        out_specs=[vmem] * 3,
        out_shape=[jax.ShapeDtypeStruct((rows, dim), F32), jax.ShapeDtypeStruct((tok, dim), BF16),
                   jax.ShapeDtypeStruct((2, dim), F32)],
        scratch_shapes=[pltpu.VMEM((2, STREAMS, group - 1, piece, dim), BF16),
                        pltpu.VMEM((4, tok, dim), BF16), pltpu.VMEM((tok, dim), BF16),
                        pltpu.VMEM((levels, 2, 8, dim), F32),
                        dma((2, STREAMS, group - 1)), dma((2, STREAMS, group - 1)),
                        dma((6,)), dma((6,)), dma((levels,)), dma((levels,))],
        compiler_params=pltpu.CompilerParams(collective_id=1, has_side_effects=True, vmem_limit_bytes=VMEM_GRANT * 4 // 5),
        cost_estimate=COST,
        name="reduce",
    )(g_att, du_win, x_in, d_hidden, gain1, g_gain2)


def whole(shape):
    return pl.BlockSpec(shape, lambda i: (0,) * len(shape))


def stepped(*shape):
    return pl.BlockSpec(shape, lambda i: (i,) + (0,) * (len(shape) - 1))


def attn_forward(x_win, gain1, gain2, w_att, cos_t, sin_t, seg_col, seg_row, tok, heads):
    win, dim = x_win.shape
    halo = (win - tok) // 2
    per = math.gcd(heads, HEADS_STEP)
    steps = heads // per
    feat = per * HEAD_DIM
    return pl.pallas_call(
        lambda *refs: attn_fwd_kernel(halo, tok, *refs),
        grid=(steps,),
        in_specs=[whole((win, dim)), whole((1, dim)), whole((1, dim)),
                  stepped(per, 4, HEAD_DIM, dim),
                  whole((HALF, win)), whole((HALF, win)), whole((win, 1)), whole((1, tok))],
        out_specs=[whole((win, dim)),
                   stepped(feat, tok),
                   stepped(feat, win),
                   stepped(feat, win),
                   stepped(feat, tok),
                   stepped(1, per, tok),
                   whole((tok, dim)), whole((tok, dim))],
        out_shape=[jax.ShapeDtypeStruct((win, dim), BF16),
                   jax.ShapeDtypeStruct((heads * HEAD_DIM, tok), BF16),
                   jax.ShapeDtypeStruct((heads * HEAD_DIM, win), BF16),
                   jax.ShapeDtypeStruct((heads * HEAD_DIM, win), BF16),
                   jax.ShapeDtypeStruct((heads * HEAD_DIM, tok), BF16),
                   jax.ShapeDtypeStruct((steps, per, tok), F32),
                   jax.ShapeDtypeStruct((tok, dim), BF16),
                   jax.ShapeDtypeStruct((tok, dim), BF16)],
        scratch_shapes=[pltpu.VMEM((win, tok), F32), pltpu.VMEM((tok, dim), F32)],
        compiler_params=pltpu.CompilerParams(dimension_semantics=("arbitrary",), vmem_limit_bytes=VMEM_GRANT),
        cost_estimate=COST,
        name="attn_fwd",
    )(x_win, gain1, gain2, w_att, cos_t, sin_t, seg_col, seg_row)


def mlp(normed2, hidden, grad_out, gain2, w_first, w_rest, rows):
    tok, dim = normed2.shape
    shards = w_rest.shape[0]
    parts = 3
    per = math.gcd(shards, MLP_SHARDS)
    block = stepped(per, parts, rows, dim)
    return pl.pallas_call(
        mlp_kernel,
        grid=(shards // per,),
        in_specs=[whole((tok, dim)), whole((tok, dim)), whole((tok, dim)), whole((1, dim)),
                  pl.BlockSpec((per, EXTRA // HEAD_DIM, HEAD_DIM, dim), lambda i: (i, w_first.shape[1] * HEAD_DIM // EXTRA - 1, 0, 0)),
                  stepped(per, w_rest.shape[1], dim)],
        out_specs=[block, whole((tok, dim)), whole((tok, dim)), whole((1, dim))],
        out_shape=[jax.ShapeDtypeStruct((shards, parts, rows, dim), BF16),
                   jax.ShapeDtypeStruct((tok, dim), BF16),
                   jax.ShapeDtypeStruct((tok, dim), BF16),
                   jax.ShapeDtypeStruct((1, dim), F32)],
        scratch_shapes=[pltpu.VMEM((tok, dim), F32), pltpu.VMEM((tok, dim), F32)],
        compiler_params=pltpu.CompilerParams(dimension_semantics=("arbitrary",), vmem_limit_bytes=VMEM_GRANT),
        cost_estimate=COST,
        name="mlp",
    )(normed2, hidden, grad_out, gain2, w_first, w_rest)


def attn_backward(u_win, d_hid, w_att, cos_t, sin_t, seg_col, seg_row, q_t, k_t, v_t, o_t, lse, heads):
    win, dim = u_win.shape
    tok = d_hid.shape[0]
    halo = (win - tok) // 2
    per = math.gcd(heads, HEADS_STEP)
    steps = heads // per
    feat = per * HEAD_DIM
    return pl.pallas_call(
        lambda *refs: attn_bwd_kernel(halo, tok, *refs),
        grid=(steps,),
        in_specs=[whole((win, dim)), whole((tok, dim)),
                  stepped(per, 4, HEAD_DIM, dim),
                  whole((HALF, win)), whole((HALF, win)), whole((win, 1)), whole((1, tok)),
                  stepped(feat, tok),
                  stepped(feat, win),
                  stepped(feat, win),
                  stepped(feat, tok),
                  stepped(1, per, tok)],
        out_specs=[stepped(per, 4, HEAD_DIM, dim), whole((win, dim))],
        out_shape=[jax.ShapeDtypeStruct((heads, 4, HEAD_DIM, dim), BF16),
                   jax.ShapeDtypeStruct((win, dim), BF16)],
        scratch_shapes=[pltpu.VMEM((win, tok), F32), pltpu.VMEM((win, dim), F32)],
        compiler_params=pltpu.CompilerParams(dimension_semantics=("arbitrary",), vmem_limit_bytes=VMEM_GRANT),
        cost_estimate=COST,
        name="attn_bwd",
    )(u_win, d_hid, w_att, cos_t, sin_t, seg_col, seg_row, q_t, k_t, v_t, o_t, lse)


def solution(mesh):
    tok_spec = P(('dp', 'tp'), None)
    seq_spec = P(('dp', 'tp'))
    in_specs = (tok_spec, seq_spec, seq_spec, P(None), P(None, None, 'tp'), P('tp', None),
                P(None), P(None, None, 'tp'), P('tp', None), tok_spec)
    out_specs = (tok_spec, tok_spec, P('dp'), P('dp', None, 'tp'), P(('dp', 'tp'), None),
                 P('dp'), P('dp', None, 'tp'), P(('dp', 'tp'), None))
    group = mesh.shape['tp']
    cols = mesh.shape['dp']

    def gather_rows(shard_rows):
        return lax.all_gather(shard_rows, 'tp', axis=0, tiled=True)

    def scatter_rows(part_sum):
        return lax.psum_scatter(part_sum, 'tp', scatter_dimension=0, tiled=True)

    def device_step(x_in, doc_ids, doc_pos, gamma1, w_qkv, w_out, gamma2, w_in, w_down, grad_out):
        tok, dim = x_in.shape
        heads_loc = w_qkv.shape[2] // HEAD_DIM
        ff_loc = w_in.shape[2]
        ff_pad = -(-ff_loc // FF_ALIGN) * FF_ALIGN
        reach = -(-MAX_DOC // tok)
        qkv_rows = jnp.transpose(w_qkv.reshape(dim, 3, heads_loc, HEAD_DIM), (2, 1, 3, 0))
        out_rows = w_out.reshape(heads_loc, 1, HEAD_DIM, dim)
        att_rows = jnp.concatenate([qkv_rows, out_rows], axis=1)
        mlp_rows = jnp.concatenate([jnp.transpose(w_in, (1, 2, 0)), w_down[None]], axis=0)
        mlp_rows = jnp.pad(mlp_rows, ((0, 0), (0, ff_pad - ff_loc), (0, 0))).reshape(3 * ff_pad, dim)
        first_rows = jnp.concatenate([att_rows.reshape(-1, dim), mlp_rows[:EXTRA]], axis=0)
        x_win, marks, w_first = collect(x_in, jnp.stack([doc_ids, doc_pos]), first_rows, cols, group, reach)
        w_rest = gather_rows(mlp_rows[EXTRA:]).reshape(group, 3 * ff_pad - EXTRA, dim)
        w_first = w_first.reshape(group, -1, HEAD_DIM, dim)
        seg_row, seg_col = doc_ids[None, :], marks[:, 0].reshape(-1, 1)
        inv_freq = 160000.0 ** (-jnp.arange(HALF, dtype=F32) / HALF)
        angle = marks[:, 1].reshape(1, -1).astype(F32) * inv_freq[:, None]
        cos_t, sin_t = jnp.cos(angle), jnp.sin(angle)


        gain1 = gamma1.astype(F32)[None, :]
        gain2 = gamma2.astype(F32)[None, :]
        u_win, q_t, k_t, v_t, o_t, lse, hidden, normed2 = attn_forward(
            x_win, gain1, gain2, w_first, cos_t, sin_t, seg_col, seg_row, tok, group * heads_loc)
        g_mlp, layer_out, d_hidden, g_gain2 = mlp(normed2, hidden, grad_out, gain2, w_first, w_rest, ff_pad)
        g_mlp = scatter_rows(g_mlp.reshape(group * 3 * ff_pad, dim))
        g_att, du_win = attn_backward(u_win, d_hidden, w_first, cos_t, sin_t, seg_col, seg_row,
                                      q_t, k_t, v_t, o_t, lse, group * heads_loc)
        g_att, grad_x, gains = reduce_rows(g_att.reshape(group, heads_loc * 4 * HEAD_DIM, dim), du_win, x_in,
                                           d_hidden, gain1, g_gain2, reach)

        g_att = g_att.reshape(heads_loc, 4, HEAD_DIM, dim)
        g_qkv = jnp.transpose(g_att[:, :3], (3, 1, 0, 2)).reshape(dim, 3, heads_loc * HEAD_DIM)
        g_out = g_att[:, 3].reshape(heads_loc * HEAD_DIM, dim)
        g_mlp = g_mlp.reshape(3, ff_pad, dim)[:, :ff_loc].astype(F32)
        g_in = jnp.transpose(g_mlp[:2], (2, 0, 1))
        return (layer_out, grad_x, gains[0], g_qkv, g_out, gains[1], g_in, g_mlp[2])

    return jax.shard_map(device_step, mesh=mesh, in_specs=in_specs, out_specs=out_specs, check_vma=False)
```
